32 devices in a mesh: pipe: 2 (over y), dp: 4 (over z), tensor: 4 (over x, core).
Axes of the slice: x: 2, y: 2, z: 4, core: 2. Of those that a mesh axis runs over, the one named last changes fastest.
Arguments:
- saved: bfloat16 [2, 2, 256, 1024], P('pipe', None, 'dp'), may hold values from -6 to 6
- top_grad: bfloat16 [2, 256, 1024], P(None, 'dp'), may hold values from -6 to 6
- gain: bfloat16 [2, 1024], P('pipe', 'dp'), may hold values from 0.25 to 1.75
- w_query: bfloat16 [2, 1024, 1536], P('pipe', 'dp', 'tensor'), may hold values from -0.1875 to 0.1875
- w_latent: bfloat16 [2, 1024, 576], P('pipe', 'dp'), may hold values from -0.1875 to 0.1875
- compressed_gain: bfloat16 [2, 512], P('pipe', 'dp'), may hold values from 0.25 to 1.75
- expand_weight: bfloat16 [2, 512, 2048], P('pipe', 'dp', 'tensor'), may hold values from -0.25 to 0.25
- w_output: bfloat16 [2, 1024, 1024], P('pipe', 'tensor', 'dp'), may hold values from -0.1875 to 0.1875
Outputs:
- input_grad: bfloat16 [2, 2, 256, 1024], P('pipe', None, ('dp', 'tensor'))
- grad_gain: float32 [2, 1024], P('pipe', 'dp')
- grad_query: float32 [2, 1024, 1536], P('pipe', 'dp', 'tensor')
- grad_latent: float32 [2, 1024, 576], P('pipe', 'dp')
- grad_latent_gain: float32 [2, 512], P('pipe', 'dp')
- grad_expand: float32 [2, 512, 2048], P('pipe', 'dp', 'tensor')
- grad_output: float32 [2, 1024, 1024], P('pipe', 'tensor', 'dp')
The draws below stay inside these ranges and needn't reach their ends.
All inputs are finite; a program needn't handle non-finite values.
Results may differ from the reference program's by a relative error of at most 0.04.
Values may be sent and summed in bfloat16 or wider, within the bound.
A program may use at most 64 MiB of HBM per device.

```python
import jax
import jax.numpy as jnp
from jax import lax

MODEL_WIDTH = 1024
NOPE = 128
ROPE = 64
VDIM = 128
COMPRESSED_RANK = 512
MB = 2
MB_TOK = 64
SECTION_COUNT = 2
TOKENS = 256
QUERY_COLUMNS = 1536
LATENT_COLUMNS = 576
EXPAND_COLUMNS = 2048
OUTPUT_ROWS = 1024
N_DP = 4
N_TENSOR = 4


def steps_of(rng, dims, pieces, low, top_value):
    def one(position, blocks):
        heights = jax.random.uniform(jax.random.fold_in(jax.random.fold_in(rng, 6), position), (blocks,), jnp.float32, low / len(pieces), top_value / len(pieces))
        return jnp.repeat(jnp.exp(heights), dims[position] // blocks).reshape((-1,) + (1,) * (len(dims) - position - 1))

    level = one(*pieces[0])
    for cut in pieces[1:]:
        level = level * one(*cut)
    return level


def normal_values(rng, dims, deviation, bound, shards=(), kind=jnp.bfloat16):
    array = jax.random.normal(rng, dims, jnp.float32) * deviation
    if len(shards) > 0:
        array = steps_of(rng, dims, shards, -0.22, 0.18) * array
    return jnp.clip(array, min=-bound, max=bound).astype(kind)


def setup_inputs(seed: int = 0) -> dict:
    seeds = jax.random.split(jax.random.key(seed), 9)
    return {
        "saved": normal_values(seeds[0], (SECTION_COUNT, MB, TOKENS, MODEL_WIDTH), 1.0, 6.0, ((0, 2), (2, 4))),
        "top_grad": normal_values(seeds[1], (MB, TOKENS, MODEL_WIDTH), 1.0, 6.0, ((1, 4),)),
        "gain": jnp.clip(1.0 + 0.15 * jax.random.normal(seeds[2], (SECTION_COUNT, MODEL_WIDTH), jnp.float32), 0.25, 1.75).astype(jnp.bfloat16),
        "w_query": normal_values(seeds[3], (SECTION_COUNT, MODEL_WIDTH, QUERY_COLUMNS), MODEL_WIDTH ** -0.5, 0.1875, ((0, 2), (1, 4), (2, 4))),
        "w_latent": normal_values(seeds[4], (SECTION_COUNT, MODEL_WIDTH, LATENT_COLUMNS), MODEL_WIDTH ** -0.5, 0.1875, ((0, 2), (1, 4))),
        "compressed_gain": jnp.clip(1.0 + 0.15 * jax.random.normal(seeds[5], (SECTION_COUNT, COMPRESSED_RANK), jnp.float32), 0.25, 1.75).astype(jnp.bfloat16),
        "expand_weight": normal_values(seeds[6], (SECTION_COUNT, COMPRESSED_RANK, EXPAND_COLUMNS), COMPRESSED_RANK ** -0.5, 0.25, ((0, 2), (1, 4), (2, 4))),
        "w_output": normal_values(seeds[7], (SECTION_COUNT, OUTPUT_ROWS, MODEL_WIDTH), OUTPUT_ROWS ** -0.5, 0.1875, ((0, 2), (1, 4), (2, 4))),
    }


EPS = 1e-06

def root_mean_scale(values, scale):
    return values * lax.rsqrt(lax.optimization_barrier(jnp.mean(values * values, axis=-1, keepdims=True)) + EPS) * scale

def rotary_angles(values):
    length = values.shape[0]
    half = values.shape[-1] // 2
    freq = jnp.exp(-jnp.log(10000.0) * jnp.arange(half, dtype=jnp.float32) / half)
    angle = jnp.arange(length, dtype=jnp.float32)[:, None] * freq[None, :]
    cosine = jnp.cos(angle)[:, None, :]
    sine = jnp.sin(angle)[:, None, :]
    first = values[..., :half]
    second = values[..., half:]
    return jnp.concatenate([first * cosine - second * sine, second * cosine + first * sine], axis=-1)

def branch(normed, w_q, w_lat, latent_norm_gain, w_exp, w_out):
    length = normed.shape[0]
    heads = w_q.shape[1] // (NOPE + ROPE)
    rounded = normed.astype(jnp.bfloat16)
    query = jnp.dot(rounded, w_q, preferred_element_type=jnp.float32).reshape(length, heads, NOPE + ROPE)
    latent_state = jnp.dot(rounded, w_lat, preferred_element_type=jnp.float32)
    compressed_state = root_mean_scale(latent_state[:, :COMPRESSED_RANK], latent_norm_gain).astype(jnp.bfloat16)
    rotary_key_part = rotary_angles(latent_state[:, None, COMPRESSED_RANK:])[:, 0, :]
    expanded = jnp.dot(compressed_state, w_exp, preferred_element_type=jnp.float32).reshape(length, heads, NOPE + VDIM)
    key_nope = expanded[:, :, :NOPE]
    values = expanded[:, :, NOPE:].astype(jnp.bfloat16)
    query_rope = rotary_angles(query[:, :, NOPE:])
    scores = jnp.einsum('qhd,khd->hqk', query[:, :, :NOPE], key_nope) + jnp.einsum('qhd,kd->hqk', query_rope, rotary_key_part)
    scores = scores * (NOPE + ROPE) ** (-0.5)
    causal = jnp.arange(length)[:, None] >= jnp.arange(length)[None, :]
    scores = jnp.where(causal[None], scores, -1e+30)
    weights = jax.nn.softmax(scores, axis=-1).astype(jnp.bfloat16)
    mixed = jnp.einsum('hqk,khd->qhd', weights.astype(jnp.float32), values.astype(jnp.float32))
    mixed = mixed.astype(jnp.bfloat16).reshape(length, heads * VDIM)
    return jnp.dot(mixed, w_out, preferred_element_type=jnp.float32)

def reference(saved, top_grad, gain, w_query, w_latent, compressed_gain, expand_weight, w_output):
    head_groups = N_TENSOR
    dgrads = []
    all_input = []
    upstream = top_grad
    for section_index in reversed(range(SECTION_COUNT)):
        gain32 = gain[section_index].astype(jnp.float32)
        lgain32 = compressed_gain[section_index].astype(jnp.float32)
        lat_w = w_latent[section_index]
        q_groups = w_query[section_index].reshape(MODEL_WIDTH, head_groups, QUERY_COLUMNS // head_groups).transpose(1, 0, 2)
        expand_groups = expand_weight[section_index].reshape(COMPRESSED_RANK, head_groups, EXPAND_COLUMNS // head_groups).transpose(1, 0, 2)
        o_groups = w_output[section_index].reshape(head_groups, OUTPUT_ROWS // head_groups, MODEL_WIDTH)

        def one_sequence(loop_carry, pair):
            x_rows, up_rows = pair
            normed, norm_pull = jax.vjp(root_mean_scale, x_rows.astype(jnp.float32), gain32)
            cot = up_rows.astype(jnp.float32)

            def one_group(wq_g, we_g, wo_g):
                unused, pull = jax.vjp(branch, normed, wq_g, lat_w, lgain32, we_g, wo_g)
                return pull(cot)
            d_norm, d_q, d_lat, d_lg, expand_gradient, d_o = jax.vmap(one_group)(q_groups, expand_groups, o_groups)
            d_normed = lax.optimization_barrier(jnp.sum(d_norm, axis=0))
            dx_norm, d_gain = norm_pull(d_normed)
            dx = (cot + dx_norm).astype(jnp.bfloat16)
            g_q = d_q.astype(jnp.float32).transpose(1, 0, 2).reshape(MODEL_WIDTH, QUERY_COLUMNS)
            expand_weight_grad = expand_gradient.astype(jnp.float32).transpose(1, 0, 2).reshape(COMPRESSED_RANK, EXPAND_COLUMNS)
            g_o = d_o.astype(jnp.float32).reshape(OUTPUT_ROWS, MODEL_WIDTH)
            g_lat = lax.optimization_barrier(jnp.sum(d_lat.astype(jnp.float32), axis=0))
            g_lg = lax.optimization_barrier(jnp.sum(d_lg, axis=0))
            loop_carry = (loop_carry[0] + d_gain, loop_carry[1] + g_q, loop_carry[2] + g_lat, loop_carry[3] + g_lg, loop_carry[4] + expand_weight_grad, loop_carry[5] + g_o)
            return (loop_carry, dx)
        loop_carry = (jnp.zeros((MODEL_WIDTH,), jnp.float32), jnp.zeros((MODEL_WIDTH, QUERY_COLUMNS), jnp.float32), jnp.zeros((MODEL_WIDTH, LATENT_COLUMNS), jnp.float32), jnp.zeros((COMPRESSED_RANK,), jnp.float32), jnp.zeros((COMPRESSED_RANK, EXPAND_COLUMNS), jnp.float32), jnp.zeros((OUTPUT_ROWS, MODEL_WIDTH), jnp.float32))
        section_inputs = []
        for micro in range(MB):
            x_seq = saved[section_index, micro].reshape(N_DP, MB_TOK, MODEL_WIDTH)
            up_seq = upstream[micro].reshape(N_DP, MB_TOK, MODEL_WIDTH)
            loop_carry, dx = lax.scan(one_sequence, loop_carry, (x_seq, up_seq))
            section_inputs.append(dx.reshape(TOKENS, MODEL_WIDTH))
        upstream = jnp.stack(section_inputs)
        all_input.append(upstream)
        dgrads.append(loop_carry)
    all_input = all_input[::-1]
    dgrads = dgrads[::-1]
    input_grad = jnp.stack(all_input)
    outs = [jnp.stack([entry[k] for entry in dgrads]) for k in range(6)]
    return (input_grad, outs[0], outs[1], outs[2], outs[3], outs[4], outs[5])
```

```python
import jax
import jax.numpy as jnp
from jax import lax
import numpy as np
from jax.experimental import pallas as pl
from jax.experimental.pallas import tpu as pltpu
from jax.sharding import PartitionSpec as P

NOPE = 128
ROPE = 64
VDIM = 128
COMPRESSED_RANK = 512


EPS = 1e-06


def passed_along(value, axis, steps):
    count = lax.axis_size(axis)
    first, last = (max(0, -steps), min(count, count - steps))
    return lax.ppermute(value, axis, [(source, source + steps) for source in range(first, last)])


def root_mean_scale(values, scale):
    return values * lax.rsqrt(jnp.mean(values * values, axis=-1, keepdims=True) + EPS) * scale


def rotary_angles(values):
    length = values.shape[0]
    half = values.shape[-1] // 2
    freq = jnp.exp(-jnp.log(10000.0) * jnp.arange(half, dtype=jnp.float32) / half)
    angle = jnp.arange(length, dtype=jnp.float32)[:, None] * freq[None, :]
    cosine = jnp.cos(angle)[:, None, :]
    sine = jnp.sin(angle)[:, None, :]
    first = values[..., :half]
    second = values[..., half:]
    return jnp.concatenate(
        [first * cosine - second * sine, second * cosine + first * sine], axis=-1
    )


def branch(normed, w_q, w_lat, latent_norm_gain, w_exp, w_out):
    length = normed.shape[0]
    heads = w_q.shape[1] // (NOPE + ROPE)
    rounded = normed.astype(jnp.bfloat16)
    query = jnp.dot(rounded, w_q, preferred_element_type=jnp.float32).reshape(
        length, heads, NOPE + ROPE
    )
    latent_state = jnp.dot(rounded, w_lat, preferred_element_type=jnp.float32)
    compressed_state = root_mean_scale(latent_state[:, :COMPRESSED_RANK], latent_norm_gain).astype(
        jnp.bfloat16
    )
    rotary_key_part = rotary_angles(latent_state[:, None, COMPRESSED_RANK:])[:, 0, :]
    expanded = jnp.dot(compressed_state, w_exp, preferred_element_type=jnp.float32).reshape(
        length, heads, NOPE + VDIM
    )
    key_nope = expanded[:, :, :NOPE]
    values = expanded[:, :, NOPE:].astype(jnp.bfloat16)
    query_rope = rotary_angles(query[:, :, NOPE:])
    scores = jnp.einsum("qhd,khd->hqk", query[:, :, :NOPE], key_nope) + jnp.einsum(
        "qhd,kd->hqk", query_rope, rotary_key_part
    )
    scores = scores * (NOPE + ROPE) ** (-0.5)
    causal = jnp.arange(length)[:, None] >= jnp.arange(length)[None, :]
    scores = jnp.where(causal[None], scores, -1e30)
    weights = jax.nn.softmax(scores, axis=-1).astype(jnp.bfloat16)
    mixed = jnp.einsum("hqk,khd->qhd", weights.astype(jnp.float32), values.astype(jnp.float32))
    mixed = mixed.astype(jnp.bfloat16).reshape(length, heads * VDIM)
    return jnp.dot(mixed, w_out, preferred_element_type=jnp.float32)


def shards(saved, top_grad, gain, w_query, w_latent, compressed_gain, expand_weight, w_output):
    gathered = (
        lax.all_gather(gain, "dp", axis=1, tiled=True),
        lax.all_gather(w_query, "dp", axis=1, tiled=True),
        lax.all_gather(w_latent, "dp", axis=1, tiled=True),
        lax.all_gather(compressed_gain, "dp", axis=1, tiled=True),
        lax.all_gather(expand_weight, "dp", axis=1, tiled=True),
        lax.all_gather(w_output, "dp", axis=2, tiled=True),
    )
    gain32 = gathered[0][0].astype(jnp.float32)
    query_all = gathered[1][0]
    latent_all = gathered[2][0]
    lgain32 = gathered[3][0].astype(jnp.float32)
    expand_all = gathered[4][0]
    output_all = gathered[5][0]
    sections = lax.axis_size("pipe")
    section_index = lax.axis_index("pipe")
    tensor_count = lax.axis_size("tensor")
    tensor_rank = lax.axis_index("tensor")
    micro_count = saved.shape[1]
    length = saved.shape[2]
    width = saved.shape[3]
    share = length // tensor_count

    def compute(normed, upstream):
        unused, pull = jax.vjp(
            lambda value: branch(value, query_all, latent_all, lgain32, expand_all, output_all),
            normed,
        )
        return pull(upstream.astype(jnp.float32))[0]

    def skip(normed, upstream):
        return jnp.zeros_like(normed)

    gain_total = jnp.zeros((width,), jnp.float32)
    results = jnp.zeros((micro_count, share, width), jnp.bfloat16)
    stored = jnp.zeros((micro_count, length, width), jnp.bfloat16)
    received = jnp.zeros((length, width), jnp.bfloat16)
    for tick in range(sections + micro_count - 1):
        micro = tick - (sections - 1 - section_index)
        active = jnp.logical_and(micro >= 0, micro < micro_count)
        picked = jnp.clip(micro, 0, micro_count - 1)
        x_rows = lax.dynamic_index_in_dim(saved[0], picked, 0, keepdims=False)
        top_rows = lax.dynamic_index_in_dim(top_grad, picked, 0, keepdims=False)
        arrived = received
        upstream = jnp.where(section_index == sections - 1, top_rows, arrived)
        x_float = x_rows.astype(jnp.float32)
        normed, norm_pull = jax.vjp(root_mean_scale, x_float, gain32)
        branch_grad = lax.cond(active, compute, skip, normed, upstream)
        d_normed = lax.psum(branch_grad.astype(jnp.bfloat16), "tensor").astype(jnp.float32)
        dx_norm, d_gain = norm_pull(d_normed)
        dx = (upstream.astype(jnp.float32) + dx_norm).astype(jnp.bfloat16)
        gain_total = gain_total + jnp.where(active, d_gain, 0.0)
        mine = lax.dynamic_slice_in_dim(dx, tensor_rank * share, share, 0)
        chosen = (jnp.arange(micro_count) == micro)[:, None, None]
        results = jnp.where(chosen, mine[None], results)
        stored = jnp.where(chosen, upstream[None], stored)
        received = passed_along(dx, "pipe", -1)
    totals = (
        jnp.zeros(query_all.shape, jnp.float32),
        jnp.zeros(latent_all.shape, jnp.float32),
        jnp.zeros(lgain32.shape, jnp.float32),
        jnp.zeros(expand_all.shape, jnp.float32),
        jnp.zeros(output_all.shape, jnp.float32),
    )
    for micro_index in range(micro_count):
        normed_again = root_mean_scale(saved[0, micro_index].astype(jnp.float32), gain32)
        unused, weight_pull = jax.vjp(
            lambda w_q, w_lat, lat_gain, w_exp, w_out: branch(
                normed_again, w_q, w_lat, lat_gain, w_exp, w_out
            ),
            query_all,
            latent_all,
            lgain32,
            expand_all,
            output_all,
        )
        cotangents = weight_pull(stored[micro_index].astype(jnp.float32))
        totals = tuple(
            (total + piece.astype(jnp.float32) for total, piece in zip(totals, cotangents))
        )
    gain_part = jnp.where(tensor_rank == 0, gain_total, 0.0)
    grad_q, grad_lat, grad_lg, grad_e, grad_o = totals
    out_q, part_lat, part_lg, out_e, out_o, part_gain = (
        lax.psum_scatter(grad_q.astype(jnp.bfloat16), "dp", scatter_dimension=0, tiled=True).astype(
            jnp.float32
        ),
        lax.psum_scatter(
            grad_lat.astype(jnp.bfloat16), "dp", scatter_dimension=0, tiled=True
        ).astype(jnp.float32),
        lax.psum_scatter(
            grad_lg.astype(jnp.bfloat16), "dp", scatter_dimension=0, tiled=True
        ).astype(jnp.float32),
        lax.psum_scatter(grad_e.astype(jnp.bfloat16), "dp", scatter_dimension=0, tiled=True).astype(
            jnp.float32
        ),
        lax.psum_scatter(grad_o.astype(jnp.bfloat16), "dp", scatter_dimension=1, tiled=True).astype(
            jnp.float32
        ),
        lax.psum_scatter(
            gain_part.astype(jnp.bfloat16), "dp", scatter_dimension=0, tiled=True
        ).astype(jnp.float32),
    )
    out_lat, out_lg, out_gain = (
        lax.psum(part_lat.astype(jnp.bfloat16), "tensor").astype(jnp.float32),
        lax.psum(part_lg.astype(jnp.bfloat16), "tensor").astype(jnp.float32),
        lax.psum(part_gain.astype(jnp.bfloat16), "tensor").astype(jnp.float32),
    )
    return (
        results[None],
        out_gain[None],
        out_q[None],
        out_lat[None],
        out_lg[None],
        out_e[None],
        out_o[None],
    )


MESH = pl.DeviceIdType.MESH
BF = jnp.bfloat16
F32 = jnp.float32


def mm(a, b):
    return lax.dot_general(a, b, (((1,), (0,)), ((), ())), preferred_element_type=F32)


def mm_nt(a, b):
    return lax.dot_general(a, b, (((1,), (1,)), ((), ())), preferred_element_type=F32)


def mm_tn(a, b):
    return lax.dot_general(a, b, (((0,), (0,)), ((), ())), preferred_element_type=F32)


def half_swap(v):
    lane = lax.broadcasted_iota(jnp.int32, v.shape, 1)
    ahead = pltpu.roll(v, v.shape[1] - ROPE // 2, 1)
    behind = pltpu.roll(v, ROPE // 2, 1)
    return jnp.where(lax.rem(lane, ROPE) < ROPE // 2, ahead, behind)


def section_kernel(
    dims,
    saved_ref, top_ref, small_ref, wq_ref, wl_ref, we_ref, wo_ref, cos_ref, sin_ref,
    ig_ref, gs_ref, gq_ref, gl_ref, ge_ref, go_ref,
    x_v, u_v, nb_v, cb_v, sm_v, wq_v, wl_v, we_v, wo_v,
    nc_v, cc_v, mx_v, uc_v, dq_v, de_v, dl_v, part_v, rs_v, dx_v, sg_v, sr_v, st_v,
    own_sem, line_s, line_r, pair_s, pair_r, dp_s, dp_r, ten_s, ten_r, pipe_s, pipe_r,
):
    n_pipe, n, n_t, micros, seq = dims
    sec, me, ten = lax.axis_index("pipe"), lax.axis_index("dp"), lax.axis_index("tensor")
    rows = micros * seq
    chunk = seq // n_t
    share = micros * chunk
    width = x_v.shape[1]
    wcol = wq_v.shape[1]
    ccol = we_v.shape[1]
    core = lax.rem(ten, 2)
    partner = ten + 1 - 2 * core
    half = wl_ref.shape[0] // 2
    drains = []

    def rcopy(a, b, ss, rs, dev):
        return pltpu.make_async_remote_copy(
            src_ref=a, dst_ref=b, send_sem=ss, recv_sem=rs, device_id=dev, device_id_type=MESH
        )

    def begin(cond, copy):
        @pl.when(cond)
        def _():
            copy.start()

        drains.append((cond, copy))

    def dp_dev(d):
        return (sec, d, ten)

    def ten_dev(d):
        return (sec, me, d)

    barrier = pltpu.get_barrier_semaphore()
    for j in range(n):
        @pl.when(j != me)
        def _():
            pl.semaphore_signal(barrier, inc=1, device_id=dp_dev(j), device_id_type=MESH)

    for j in range(n_t):
        @pl.when(j != ten)
        def _():
            pl.semaphore_signal(barrier, inc=1, device_id=ten_dev(j), device_id_type=MESH)

        @pl.when(sec > 0)
        def _():
            pl.semaphore_signal(barrier, inc=1, device_id=(sec - 1, me, j), device_id_type=MESH)

        @pl.when(sec < n_pipe - 1)
        def _():
            pl.semaphore_signal(barrier, inc=1, device_id=(sec + 1, me, j), device_id_type=MESH)

    neighbours = jnp.minimum(sec, 1) + jnp.minimum(n_pipe - 1 - sec, 1)
    pl.semaphore_wait(barrier, n - 1 + n_t - 1 + neighbours * n_t)

    def line_start(k, source, at):
        begin(me < n - 1, rcopy(source, at(me), line_s.at[k, 0, 0], line_r.at[k, me], dp_dev(me + 1)))
        begin(me > 0, rcopy(source, at(me), line_s.at[k, 1, 0], line_r.at[k, me], dp_dev(me - 1)))

    def line_step(k, at, s, extra=None):
        for way, block, valid, more, dest in (
            (0, jnp.maximum(me - 1 - s, 0), me - 1 - s >= 0, me < n - 1, me + 1),
            (1, jnp.minimum(me + 1 + s, n - 1), me + 1 + s <= n - 1, me > 0, me - 1),
        ):
            arrived = rcopy(at(block), at(block), line_s.at[k, way, s + 1], line_r.at[k, block], dp_dev(dest))

            @pl.when(valid)
            def _():
                arrived.wait_recv()

            if s < n - 2:
                begin(jnp.logical_and(valid, more), arrived)
            if extra is not None:
                extra(block, valid, way, s)

    def spread_dp(k, source, dest):
        for j in range(n):
            begin(j != me, rcopy(source(j), dest.at[me], dp_s.at[k, j], dp_r.at[k, me], dp_dev(j)))

    def collect_dp(k, dest):
        for j in range(n):
            @pl.when(j != me)
            def _():
                rcopy(dest.at[j], dest.at[j], dp_s.at[k, j], dp_r.at[k, j], dp_dev(j)).wait_recv()

    def spread_ten(k, source, dest):
        for j in range(n_t):
            begin(j != ten, rcopy(source(j), dest.at[ten], ten_s.at[k, j], ten_r.at[k, ten], ten_dev(j)))

    def collect_ten(k, dest):
        for j in range(n_t):
            @pl.when(j != ten)
            def _():
                rcopy(dest.at[j], dest.at[j], ten_s.at[k, j], ten_r.at[k, j], ten_dev(j)).wait_recv()

    wq_at = lambda b: wq_v.at[b]
    wl_at = lambda b: wl_v.at[b, core]
    we_at = lambda b: we_v.at[b]
    wo_at = lambda b: wo_v.at[b]
    dq_at = lambda b: dq_v.at[b]
    de_at = lambda b: de_v.at[b]
    dl_at = lambda b: dl_v.at[ten, b]

    spread_dp(0, lambda j: small_ref, sm_v)
    line_start(0, wq_ref, wq_at)
    line_start(1, wl_ref.at[pl.ds(pl.multiple_of(core * half, half), half)], wl_at)
    line_start(2, we_ref, we_at)
    line_start(3, wo_ref, wo_at)
    owns = [
        pltpu.make_async_copy(wq_ref, wq_v.at[me], own_sem.at[0]),
        pltpu.make_async_copy(wl_ref.at[pl.ds(0, half)], wl_v.at[me, 0], own_sem.at[1]),
        pltpu.make_async_copy(wl_ref.at[pl.ds(half, half)], wl_v.at[me, 1], own_sem.at[2]),
        pltpu.make_async_copy(we_ref, we_v.at[me], own_sem.at[3]),
        pltpu.make_async_copy(wo_ref, wo_v.at[me], own_sem.at[4]),
        pltpu.make_async_copy(small_ref, sm_v.at[me], own_sem.at[5]),
    ]
    for copy in owns:
        copy.start()

    for j in range(n_t):
        for m in range(micros):
            x_v[j * share + m * chunk : j * share + (m + 1) * chunk] = saved_ref[
                m, j * chunk : (j + 1) * chunk
            ]
    for copy in owns:
        copy.wait()
    collect_dp(0, sm_v)
    gain = jnp.concatenate([sm_v[d][0:1, :wcol] for d in range(n)], axis=1)
    lgain = jnp.concatenate([sm_v[d][0:1, wcol : wcol + ccol] for d in range(n)], axis=1)
    x32 = x_v[...].astype(F32)
    r = lax.rsqrt(jnp.mean(x32 * x32, axis=1, keepdims=True) + EPS)
    nb = (x32 * r * gain).astype(BF)
    nb_v[...] = nb

    pair_copies = []

    def to_partner(block, valid, way, s):
        copy = rcopy(wl_v.at[block, core], wl_v.at[block, core], pair_s.at[block], pair_r.at[block], ten_dev(partner))
        begin(valid, copy)
        pair_copies.append((valid, block))

    for s in range(n - 1):
        line_step(0, wq_at, s)
        line_step(1, wl_at, s, to_partner)
        line_step(2, we_at, s)
        line_step(3, wo_at, s)
    for valid, block in pair_copies:
        @pl.when(valid)
        def _(block=block):
            rcopy(
                wl_v.at[block, 1 - core], wl_v.at[block, 1 - core], pair_s.at[block], pair_r.at[block], ten_dev(partner)
            ).wait_recv()

    wq = wq_v[...].reshape(width, wq_v.shape[2])
    wl = wl_v[...].reshape(width, wl_v.shape[3])
    we = we_v[...].reshape(n * ccol, we_v.shape[2])
    q = mm(nb, wq)
    lat = mm(nb, wl)
    rank = n * ccol
    l32 = lat[:, :rank]
    rl = lax.rsqrt(jnp.mean(l32 * l32, axis=1, keepdims=True) + EPS)
    cb = (l32 * rl * lgain).astype(BF)
    cb_v[...] = cb
    spread_dp(1, lambda j: nb_v.at[:, pl.ds(j * wcol, wcol)], nc_v)
    spread_dp(2, lambda j: cb_v.at[:, pl.ds(j * ccol, ccol)], cc_v)
    ex = mm(cb, we)
    cosine, sine = cos_ref[...], sin_ref[...]
    lr = lat[:, rank:]
    lr2 = jnp.concatenate([lr, lr], axis=1)
    rk = (lr2 * cosine + half_swap(lr2) * sine).astype(BF)
    qr_all = q[:, 2 * NOPE :]
    qr = qr_all * cosine + half_swap(qr_all) * sine
    lane = lax.broadcasted_iota(jnp.int32, qr.shape, 1)
    row = lax.broadcasted_iota(jnp.int32, (rows, rows), 0)
    col = lax.broadcasted_iota(jnp.int32, (rows, rows), 1)

    def place(i):
        return (i // share) * chunk + lax.rem(i, chunk)

    same = lax.rem(row, share) // chunk == lax.rem(col, share) // chunk
    keep = jnp.logical_and(same, place(row) >= place(col))
    scale = (NOPE + ROPE) ** (-0.5)
    heads = []
    for h in range(2):
        qn = q[:, h * NOPE : (h + 1) * NOPE].astype(BF)
        kn = ex[:, h * (NOPE + VDIM) : h * (NOPE + VDIM) + NOPE].astype(BF)
        vv = ex[:, h * (NOPE + VDIM) + NOPE : (h + 1) * (NOPE + VDIM)].astype(BF)
        mask = lane < ROPE if h == 0 else lane >= ROPE
        qh = jnp.where(mask, qr, 0.0).astype(BF)
        scores = (mm_nt(qn, kn) + mm_nt(qh, rk)) * scale
        scores = jnp.where(keep, scores, -1e30)
        e = jnp.exp(scores - jnp.max(scores, axis=1, keepdims=True))
        w32 = e / jnp.sum(e, axis=1, keepdims=True)
        wb = w32.astype(BF)
        mx_v[me, :, h * VDIM : (h + 1) * VDIM] = mm(wb, vv).astype(BF)
        heads.append((qn, kn, vv, mask, qh, w32, wb))
    spread_dp(3, lambda j: mx_v.at[me], mx_v)
    for j in range(n):
        @pl.when(j == me)
        def _():
            nc_v[j] = nb_v[:, j * wcol : (j + 1) * wcol]
            cc_v[j] = cb_v[:, j * ccol : (j + 1) * ccol]

    @pl.when(sec == n_pipe - 1)
    def _():
        for j in range(n_t):
            for m in range(micros):
                u_v[j, m * chunk : (m + 1) * chunk] = top_ref[m, j * chunk : (j + 1) * chunk]

    for j in range(n_t):
        @pl.when(sec < n_pipe - 1)
        def _():
            rcopy(
                u_v.at[j], u_v.at[j], pipe_s.at[j], pipe_r.at[j], (jnp.minimum(sec + 1, n_pipe - 1), me, j)
            ).wait_recv()

    ub = u_v[...].reshape(rows, width)
    for j in range(n):
        uc_v[1, j] = ub[:, j * wcol : (j + 1) * wcol]
    spread_dp(4, lambda j: uc_v.at[1, j], uc_v.at[0])
    uc_v[0, me] = uc_v[1, me]
    dm = jnp.zeros((rows, wo_v.shape[1]), F32)
    for j in range(n):
        dm = dm + mm_nt(ub[:, j * wcol : (j + 1) * wcol], wo_v[j])
    dm = dm.astype(BF)
    dqr = jnp.zeros((rows, 2 * ROPE), F32)
    drk = jnp.zeros((rows, 2 * ROPE), F32)
    for h, (qn, kn, vv, mask, qh, w32, wb) in enumerate(heads):
        dmh = dm[:, h * VDIM : (h + 1) * VDIM]
        dv = mm_tn(wb, dmh)
        dw = mm_nt(dmh, vv).astype(BF).astype(F32)
        ds = (w32 * (dw - jnp.sum(dw * w32, axis=1, keepdims=True)) * scale).astype(BF)
        dq_v[me, :, h * NOPE : (h + 1) * NOPE] = mm(ds, kn).astype(BF)
        dqr = dqr + jnp.where(mask, mm(ds, rk), 0.0)
        drk = drk + mm_tn(ds, qh)
        de_v[me, :, h * (NOPE + VDIM) : h * (NOPE + VDIM) + NOPE] = mm_tn(ds, qn).astype(BF)
        de_v[me, :, h * (NOPE + VDIM) + NOPE : (h + 1) * (NOPE + VDIM)] = dv.astype(BF)
    dq_v[me, :, 2 * NOPE :] = (dqr * cosine - half_swap(dqr) * sine).astype(BF)
    drk = drk * cosine - half_swap(drk) * sine
    drk = drk + pltpu.roll(drk, ROPE, 1)
    line_start(4, dq_v.at[me], dq_at)
    line_start(5, de_v.at[me], de_at)
    dc = mm_nt(de_v[me], we)
    dlg = jnp.sum(dc * l32 * rl, axis=0, keepdims=True)
    dcg = dc * lgain
    dl = rl * dcg - l32 * (rl * rl * rl) * jnp.mean(l32 * dcg, axis=1, keepdims=True)
    dlat = jnp.concatenate([dl.astype(BF), drk[:, :ROPE].astype(BF)], axis=1)
    dn = mm_nt(dq_v[me], wq) + mm_nt(dlat, wl)
    part_v[:, :, :width] = dn.astype(BF).reshape(n_t, share, width)
    part_v[:, :, width:] = dlat.reshape(n_t, share, dlat.shape[1])
    spread_ten(0, lambda j: part_v.at[j], rs_v)
    rs_v[ten] = part_v[ten]
    collect_ten(0, rs_v)
    total = jnp.sum(rs_v[...].astype(F32), axis=0)
    dns = total[:, :width]
    x_my = x_v[pl.ds(pl.multiple_of(ten * share, share), share)].astype(F32)
    r_my = lax.rsqrt(jnp.mean(x_my * x_my, axis=1, keepdims=True) + EPS)
    dng = dns * gain
    u_my = u_v[ten].astype(F32)
    dx = u_my + r_my * dng - x_my * (r_my * r_my * r_my) * jnp.mean(x_my * dng, axis=1, keepdims=True)
    dx_v[...] = dx.astype(BF)
    for j in range(n_t):
        begin(sec > 0, rcopy(dx_v, u_v.at[ten], pipe_s.at[j], pipe_r.at[ten], (jnp.maximum(sec - 1, 0), me, j)))
    dl_v[ten, me] = total[:, width:].astype(BF)
    line_start(6, dl_v.at[ten, me], dl_at)
    dgain = jnp.sum(dns * x_my * r_my, axis=0, keepdims=True)
    for j in range(n):
        piece = jnp.concatenate(
            [dgain[:, j * wcol : (j + 1) * wcol], dlg[:, j * ccol : (j + 1) * ccol]], axis=1
        )
        sg_v[j] = jnp.broadcast_to(piece, sg_v.shape[1:])
    spread_dp(5, lambda j: sg_v.at[j], sr_v)
    sr_v[me] = sg_v[me]
    for m in range(micros):
        ig_ref[m] = dx[m * chunk : (m + 1) * chunk].astype(BF)
    for s in range(n - 1):
        line_step(4, dq_at, s)
        line_step(5, de_at, s)
        line_step(6, dl_at, s)
    spread_ten(1, lambda j: dl_v.at[ten], dl_v)
    collect_dp(5, sr_v)
    st_v[ten] = jnp.sum(sr_v[...], axis=0)
    spread_ten(2, lambda j: st_v.at[ten], st_v)
    collect_dp(1, nc_v)
    collect_dp(2, cc_v)
    collect_dp(3, mx_v)
    collect_dp(4, uc_v.at[0])
    nc = nc_v[...].reshape(n * rows, wcol)
    gq_ref[...] = mm_tn(nc, dq_v[...].reshape(n * rows, dq_v.shape[2]))
    ge_ref[...] = mm_tn(cc_v[...].reshape(n * rows, ccol), de_v[...].reshape(n * rows, de_v.shape[2]))
    go_ref[...] = mm_tn(mx_v[...].reshape(n * rows, mx_v.shape[2]), uc_v[0].reshape(n * rows, wcol))
    collect_ten(1, dl_v)
    acc = jnp.zeros(gl_ref.shape, F32)
    for d in range(n):
        block = jnp.concatenate([dl_v[j, d] for j in range(n_t)], axis=0)
        acc = acc + mm_tn(nc_v[d], block)
    gl_ref[...] = acc
    collect_ten(2, st_v)
    gs_ref[...] = jnp.sum(st_v[...], axis=0)
    for cond, copy in drains:
        @pl.when(cond)
        def _(copy=copy):
            copy.wait_send()


def section_step(saved, top_grad, gain, w_query, w_latent, compressed_gain, expand_weight, w_output):
    n_pipe, n, n_t = (lax.axis_size(a) for a in ("pipe", "dp", "tensor"))
    micros, seq, width = saved.shape[1:]
    wcol, ccol = gain.shape[1], compressed_gain.shape[1]
    rows, share = micros * seq, micros * seq // n_t
    qcols, lcols = w_query.shape[2], w_latent.shape[2]
    ecols, orows = expand_weight.shape[2], w_output.shape[1]
    small = jnp.concatenate([gain, compressed_gain], axis=1).astype(F32)
    small = jnp.broadcast_to(small, (8, wcol + ccol))
    per = NOPE + ROPE
    wq = w_query[0]
    wq = jnp.concatenate(
        [wq[:, :NOPE], wq[:, per : per + NOPE], wq[:, NOPE:per], wq[:, per + NOPE :]], axis=1
    )
    order = np.arange(rows)
    place = (order // share) * (seq // n_t) + order % (seq // n_t)
    pair = np.arange(2 * ROPE) % (ROPE // 2)
    angle = place[:, None] * np.exp(-np.log(10000.0) * pair / (ROPE // 2))[None, :]
    sign = np.where(np.arange(2 * ROPE) % ROPE < ROPE // 2, -1.0, 1.0)
    cosine = jnp.asarray(np.cos(angle), F32)
    sine = jnp.asarray(np.sin(angle) * sign, F32)
    vm = pl.BlockSpec(memory_space=pltpu.VMEM)
    shape = jax.ShapeDtypeStruct
    dma = pltpu.SemaphoreType.DMA
    ig, gs, gq, gl, ge, go = pl.pallas_call(
        lambda *refs: section_kernel((n_pipe, n, n_t, micros, seq), *refs),
        name="section_step",
        out_shape=(
            shape((micros, seq // n_t, width), BF),
            shape((8, wcol + ccol), F32),
            shape((wcol, qcols), F32),
            shape((wcol, lcols), F32),
            shape((ccol, ecols), F32),
            shape((orows, wcol), F32),
        ),
        in_specs=[vm] * 9,
        out_specs=(vm,) * 6,
        scratch_shapes=[
            pltpu.VMEM((rows, width), BF),
            pltpu.VMEM((n_t, share, width), BF),
            pltpu.VMEM((rows, width), BF),
            pltpu.VMEM((rows, n * ccol), BF),
            pltpu.VMEM((n, 8, wcol + ccol), F32),
            pltpu.VMEM((n, wcol, qcols), BF),
            pltpu.VMEM((n, 2, wcol // 2, lcols), BF),
            pltpu.VMEM((n, ccol, ecols), BF),
            pltpu.VMEM((n, orows, wcol), BF),
            pltpu.VMEM((n, rows, wcol), BF),
            pltpu.VMEM((n, rows, ccol), BF),
            pltpu.VMEM((n, rows, orows), BF),
            pltpu.VMEM((2, n, rows, wcol), BF),
            pltpu.VMEM((n, rows, qcols), BF),
            pltpu.VMEM((n, rows, ecols), BF),
            pltpu.VMEM((n_t, n, share, lcols), BF),
            pltpu.VMEM((n_t, share, width + lcols), BF),
            pltpu.VMEM((n_t, share, width + lcols), BF),
            pltpu.VMEM((share, width), BF),
            pltpu.VMEM((n, 8, wcol + ccol), F32),
            pltpu.VMEM((n, 8, wcol + ccol), F32),
            pltpu.VMEM((n_t, 8, wcol + ccol), F32),
            dma((6,)),
            dma((7, 2, n)),
            dma((7, n)),
            dma((n,)),
            dma((n,)),
            dma((6, n)),
            dma((6, n)),
            dma((3, n_t)),
            dma((3, n_t)),
            dma((n_t,)),
            dma((n_t,)),
        ],
        compiler_params=pltpu.CompilerParams(
            collective_id=0, has_side_effects=True, vmem_limit_bytes=60 * 1024 * 1024
        ),
    )(saved[0], top_grad, small, wq, w_latent[0], expand_weight[0], w_output[0], cosine, sine)
    gq = jnp.concatenate(
        [gq[:, :NOPE], gq[:, 2 * NOPE : 2 * NOPE + ROPE], gq[:, NOPE : 2 * NOPE], gq[:, 2 * NOPE + ROPE :]],
        axis=1,
    )
    return (
        ig[None],
        gs[0:1, :wcol],
        gq[None],
        gl[None],
        gs[0:1, wcol:],
        ge[None],
        go[None],
    )


def choose(saved, top_grad, gain, w_query, w_latent, compressed_gain, expand_weight, w_output):
    arrays = (saved, top_grad, gain, w_query, w_latent, compressed_gain, expand_weight, w_output)
    n_t = lax.axis_size("tensor")
    fits = (
        lax.axis_size("dp") > 1
        and n_t % 2 == 0
        and w_query.shape[2] == 2 * (NOPE + ROPE)
        and gain.shape[1] % 128 == 0
        and compressed_gain.shape[1] % 128 == 0
        and saved.shape[2] % (16 * n_t) == 0
    )
    return section_step(*arrays) if fits else shards(*arrays)


def solution(mesh):
    in_specs = (
        P("pipe", None, "dp", None),
        P(None, "dp", None),
        P("pipe", "dp"),
        P("pipe", "dp", "tensor"),
        P("pipe", "dp", None),
        P("pipe", "dp"),
        P("pipe", "dp", "tensor"),
        P("pipe", "tensor", "dp"),
    )
    out_specs = (
        P("pipe", None, ("dp", "tensor"), None),
        P("pipe", "dp"),
        P("pipe", "dp", "tensor"),
        P("pipe", "dp", None),
        P("pipe", "dp"),
        P("pipe", "dp", "tensor"),
        P("pipe", "tensor", "dp"),
    )
    return jax.shard_map(choose, mesh=mesh, in_specs=in_specs, out_specs=out_specs, check_vma=False)
```

```python
import jax
import jax.numpy as jnp
from jax import lax
import numpy as np
from jax.experimental import pallas as pl
from jax.experimental.pallas import tpu as pltpu
from jax.sharding import PartitionSpec as P

NOPE = 128
ROPE = 64
VDIM = 128
COMPRESSED_RANK = 512


EPS = 1e-06


def passed_along(value, axis, steps):
    count = lax.axis_size(axis)
    first, last = (max(0, -steps), min(count, count - steps))
    return lax.ppermute(value, axis, [(source, source + steps) for source in range(first, last)])


def root_mean_scale(values, scale):
    return values * lax.rsqrt(jnp.mean(values * values, axis=-1, keepdims=True) + EPS) * scale


def rotary_angles(values):
    length = values.shape[0]
    half = values.shape[-1] // 2
    freq = jnp.exp(-jnp.log(10000.0) * jnp.arange(half, dtype=jnp.float32) / half)
    angle = jnp.arange(length, dtype=jnp.float32)[:, None] * freq[None, :]
    cosine = jnp.cos(angle)[:, None, :]
    sine = jnp.sin(angle)[:, None, :]
    first = values[..., :half]
    second = values[..., half:]
    return jnp.concatenate(
        [first * cosine - second * sine, second * cosine + first * sine], axis=-1
    )


def branch(normed, w_q, w_lat, latent_norm_gain, w_exp, w_out):
    length = normed.shape[0]
    heads = w_q.shape[1] // (NOPE + ROPE)
    rounded = normed.astype(jnp.bfloat16)
    query = jnp.dot(rounded, w_q, preferred_element_type=jnp.float32).reshape(
        length, heads, NOPE + ROPE
    )
    latent_state = jnp.dot(rounded, w_lat, preferred_element_type=jnp.float32)
    compressed_state = root_mean_scale(latent_state[:, :COMPRESSED_RANK], latent_norm_gain).astype(
        jnp.bfloat16
    )
    rotary_key_part = rotary_angles(latent_state[:, None, COMPRESSED_RANK:])[:, 0, :]
    expanded = jnp.dot(compressed_state, w_exp, preferred_element_type=jnp.float32).reshape(
        length, heads, NOPE + VDIM
    )
    key_nope = expanded[:, :, :NOPE]
    values = expanded[:, :, NOPE:].astype(jnp.bfloat16)
    query_rope = rotary_angles(query[:, :, NOPE:])
    scores = jnp.einsum("qhd,khd->hqk", query[:, :, :NOPE], key_nope) + jnp.einsum(
        "qhd,kd->hqk", query_rope, rotary_key_part
    )
    scores = scores * (NOPE + ROPE) ** (-0.5)
    causal = jnp.arange(length)[:, None] >= jnp.arange(length)[None, :]
    scores = jnp.where(causal[None], scores, -1e30)
    weights = jax.nn.softmax(scores, axis=-1).astype(jnp.bfloat16)
    mixed = jnp.einsum("hqk,khd->qhd", weights.astype(jnp.float32), values.astype(jnp.float32))
    mixed = mixed.astype(jnp.bfloat16).reshape(length, heads * VDIM)
    return jnp.dot(mixed, w_out, preferred_element_type=jnp.float32)


def shards(saved, top_grad, gain, w_query, w_latent, compressed_gain, expand_weight, w_output):
    gathered = (
        lax.all_gather(gain, "dp", axis=1, tiled=True),
        lax.all_gather(w_query, "dp", axis=1, tiled=True),
        lax.all_gather(w_latent, "dp", axis=1, tiled=True),
        lax.all_gather(compressed_gain, "dp", axis=1, tiled=True),
        lax.all_gather(expand_weight, "dp", axis=1, tiled=True),
        lax.all_gather(w_output, "dp", axis=2, tiled=True),
    )
    gain32 = gathered[0][0].astype(jnp.float32)
    query_all = gathered[1][0]
    latent_all = gathered[2][0]
    lgain32 = gathered[3][0].astype(jnp.float32)
    expand_all = gathered[4][0]
    output_all = gathered[5][0]
    sections = lax.axis_size("pipe")
    section_index = lax.axis_index("pipe")
    tensor_count = lax.axis_size("tensor")
    tensor_rank = lax.axis_index("tensor")
    micro_count = saved.shape[1]
    length = saved.shape[2]
    width = saved.shape[3]
    share = length // tensor_count

    def compute(normed, upstream):
        unused, pull = jax.vjp(
            lambda value: branch(value, query_all, latent_all, lgain32, expand_all, output_all),
            normed,
        )
        return pull(upstream.astype(jnp.float32))[0]

    def skip(normed, upstream):
        return jnp.zeros_like(normed)

    gain_total = jnp.zeros((width,), jnp.float32)
    results = jnp.zeros((micro_count, share, width), jnp.bfloat16)
    stored = jnp.zeros((micro_count, length, width), jnp.bfloat16)
    received = jnp.zeros((length, width), jnp.bfloat16)
    for tick in range(sections + micro_count - 1):
        micro = tick - (sections - 1 - section_index)
        active = jnp.logical_and(micro >= 0, micro < micro_count)
        picked = jnp.clip(micro, 0, micro_count - 1)
        x_rows = lax.dynamic_index_in_dim(saved[0], picked, 0, keepdims=False)
        top_rows = lax.dynamic_index_in_dim(top_grad, picked, 0, keepdims=False)
        arrived = received
        upstream = jnp.where(section_index == sections - 1, top_rows, arrived)
        x_float = x_rows.astype(jnp.float32)
        normed, norm_pull = jax.vjp(root_mean_scale, x_float, gain32)
        branch_grad = lax.cond(active, compute, skip, normed, upstream)
        d_normed = lax.psum(branch_grad.astype(jnp.bfloat16), "tensor").astype(jnp.float32)
        dx_norm, d_gain = norm_pull(d_normed)
        dx = (upstream.astype(jnp.float32) + dx_norm).astype(jnp.bfloat16)
        gain_total = gain_total + jnp.where(active, d_gain, 0.0)
        mine = lax.dynamic_slice_in_dim(dx, tensor_rank * share, share, 0)
        chosen = (jnp.arange(micro_count) == micro)[:, None, None]
        results = jnp.where(chosen, mine[None], results)
        stored = jnp.where(chosen, upstream[None], stored)
        received = passed_along(dx, "pipe", -1)
    totals = (
        jnp.zeros(query_all.shape, jnp.float32),
        jnp.zeros(latent_all.shape, jnp.float32),
        jnp.zeros(lgain32.shape, jnp.float32),
        jnp.zeros(expand_all.shape, jnp.float32),
        jnp.zeros(output_all.shape, jnp.float32),
    )
    for micro_index in range(micro_count):
        normed_again = root_mean_scale(saved[0, micro_index].astype(jnp.float32), gain32)
        unused, weight_pull = jax.vjp(
            lambda w_q, w_lat, lat_gain, w_exp, w_out: branch(
                normed_again, w_q, w_lat, lat_gain, w_exp, w_out
            ),
            query_all,
            latent_all,
            lgain32,
            expand_all,
            output_all,
        )
        cotangents = weight_pull(stored[micro_index].astype(jnp.float32))
        totals = tuple(
            (total + piece.astype(jnp.float32) for total, piece in zip(totals, cotangents))
        )
    gain_part = jnp.where(tensor_rank == 0, gain_total, 0.0)
    grad_q, grad_lat, grad_lg, grad_e, grad_o = totals
    out_q, part_lat, part_lg, out_e, out_o, part_gain = (
        lax.psum_scatter(grad_q.astype(jnp.bfloat16), "dp", scatter_dimension=0, tiled=True).astype(
            jnp.float32
        ),
        lax.psum_scatter(
            grad_lat.astype(jnp.bfloat16), "dp", scatter_dimension=0, tiled=True
        ).astype(jnp.float32),
        lax.psum_scatter(
            grad_lg.astype(jnp.bfloat16), "dp", scatter_dimension=0, tiled=True
        ).astype(jnp.float32),
        lax.psum_scatter(grad_e.astype(jnp.bfloat16), "dp", scatter_dimension=0, tiled=True).astype(
            jnp.float32
        ),
        lax.psum_scatter(grad_o.astype(jnp.bfloat16), "dp", scatter_dimension=1, tiled=True).astype(
            jnp.float32
        ),
        lax.psum_scatter(
            gain_part.astype(jnp.bfloat16), "dp", scatter_dimension=0, tiled=True
        ).astype(jnp.float32),
    )
    out_lat, out_lg, out_gain = (
        lax.psum(part_lat.astype(jnp.bfloat16), "tensor").astype(jnp.float32),
        lax.psum(part_lg.astype(jnp.bfloat16), "tensor").astype(jnp.float32),
        lax.psum(part_gain.astype(jnp.bfloat16), "tensor").astype(jnp.float32),
    )
    return (
        results[None],
        out_gain[None],
        out_q[None],
        out_lat[None],
        out_lg[None],
        out_e[None],
        out_o[None],
    )


MESH = pl.DeviceIdType.MESH
BF = jnp.bfloat16
F32 = jnp.float32


def mm(a, b):
    return lax.dot_general(a, b, (((1,), (0,)), ((), ())), preferred_element_type=F32)


def mm_nt(a, b):
    return lax.dot_general(a, b, (((1,), (1,)), ((), ())), preferred_element_type=F32)


def mm_tn(a, b):
    return lax.dot_general(a, b, (((0,), (0,)), ((), ())), preferred_element_type=F32)


def half_swap(v):
    lane = lax.broadcasted_iota(jnp.int32, v.shape, 1)
    ahead = pltpu.roll(v, v.shape[1] - ROPE // 2, 1)
    behind = pltpu.roll(v, ROPE // 2, 1)
    return jnp.where(lax.rem(lane, ROPE) < ROPE // 2, ahead, behind)


def section_kernel(
    dims,
    saved_ref, top_ref, gain_ref, lgain_ref, wq_ref, wl_ref, we_ref, wo_ref, cos_ref, sin_ref,
    ig_ref, gg_ref, gq_ref, gl_ref, glg_ref, ge_ref, go_ref,
    x_v, own_v, u_v, nb_v, cb_v, sm_v, wq_v, wl_v, we_v, wo_v,
    nc_v, cc_v, mx_v, uc_v, dq_v, de_v, dl_v, part_v, rs_v, lp_v, ls_v, q_v, lat_v, dx_v, sg_v, sr_v, st_v,
    own_sem, line_s, line_r, pair_s, pair_r, dp_s, dp_r, ten_s, ten_r, pipe_s, pipe_r, lat_s, lat_r,
):
    n_pipe, n, n_t, micros, seq = dims
    sec, me, ten = lax.axis_index("pipe"), lax.axis_index("dp"), lax.axis_index("tensor")
    rows = micros * seq
    chunk = seq // n_t
    share = micros * chunk
    width = x_v.shape[1]
    wcol = wq_v.shape[1]
    ccol = we_v.shape[1]
    core = lax.rem(ten, 2)
    partner = ten + 1 - 2 * core
    half = wl_ref.shape[0] // 2
    drains = []

    def rcopy(a, b, ss, rs, dev):
        return pltpu.make_async_remote_copy(
            src_ref=a, dst_ref=b, send_sem=ss, recv_sem=rs, device_id=dev, device_id_type=MESH
        )

    def begin(cond, copy):
        @pl.when(cond)
        def _():
            copy.start()

        drains.append((cond, copy))

    def dp_dev(d):
        return (sec, d, ten)

    def ten_dev(d):
        return (sec, me, d)

    barrier = pltpu.get_barrier_semaphore()
    for j in range(n):
        @pl.when(j != me)
        def _():
            pl.semaphore_signal(barrier, inc=1, device_id=dp_dev(j), device_id_type=MESH)

    for j in range(n_t):
        @pl.when(j != ten)
        def _():
            pl.semaphore_signal(barrier, inc=1, device_id=ten_dev(j), device_id_type=MESH)

        @pl.when(sec > 0)
        def _():
            pl.semaphore_signal(barrier, inc=1, device_id=(sec - 1, me, j), device_id_type=MESH)

        @pl.when(sec < n_pipe - 1)
        def _():
            pl.semaphore_signal(barrier, inc=1, device_id=(sec + 1, me, j), device_id_type=MESH)

    neighbours = jnp.minimum(sec, 1) + jnp.minimum(n_pipe - 1 - sec, 1)
    pl.semaphore_wait(barrier, n - 1 + n_t - 1 + neighbours * n_t)

    def line_start(k, source, at):
        begin(me < n - 1, rcopy(source, at(me), line_s.at[k, 0, 0], line_r.at[k, me], dp_dev(me + 1)))
        begin(me > 0, rcopy(source, at(me), line_s.at[k, 1, 0], line_r.at[k, me], dp_dev(me - 1)))

    def line_step(k, at, s, extra=None, gate=None):
        for way, block, valid, more, dest in (
            (0, jnp.maximum(me - 1 - s, 0), me - 1 - s >= 0, me < n - 1, me + 1),
            (1, jnp.minimum(me + 1 + s, n - 1), me + 1 + s <= n - 1, me > 0, me - 1),
        ):
            if gate is not None:
                valid = jnp.logical_and(valid, gate)
            arrived = rcopy(at(block), at(block), line_s.at[k, way, s + 1], line_r.at[k, block], dp_dev(dest))

            @pl.when(valid)
            def _():
                arrived.wait_recv()

            if s < n - 2:
                begin(jnp.logical_and(valid, more), arrived)
            if extra is not None:
                extra(block, valid, way, s)

    def spread_dp(k, source, dest):
        for j in range(n):
            begin(j != me, rcopy(source(j), dest.at[me], dp_s.at[k, j], dp_r.at[k, me], dp_dev(j)))

    def collect_dp(k, dest):
        for j in range(n):
            @pl.when(j != me)
            def _():
                rcopy(dest.at[j], dest.at[j], dp_s.at[k, j], dp_r.at[k, j], dp_dev(j)).wait_recv()

    def spread_ten(k, source, dest):
        for j in range(n_t):
            begin(j != ten, rcopy(source(j), dest.at[ten], ten_s.at[k, j], ten_r.at[k, ten], ten_dev(j)))

    def collect_ten(k, dest):
        for j in range(n_t):
            @pl.when(j != ten)
            def _():
                rcopy(dest.at[j], dest.at[j], ten_s.at[k, j], ten_r.at[k, j], ten_dev(j)).wait_recv()

    wq_at = lambda b: wq_v.at[b]
    wl_at = lambda b: wl_v.at[b, core]
    we_at = lambda b: we_v.at[b]
    wo_at = lambda b: wo_v.at[b]
    dq_at = lambda b: dq_v.at[b]
    de_at = lambda b: de_v.at[b]
    dl_at = lambda b: dl_v.at[ten, b]

    own_v[:, :wcol] = jnp.broadcast_to(gain_ref[...].astype(F32), (8, wcol))
    own_v[:, wcol:] = jnp.broadcast_to(lgain_ref[...].astype(F32), (8, ccol))
    spread_dp(0, lambda j: own_v, sm_v)
    sm_v[me] = own_v[...]
    line_start(0, wq_ref, wq_at)
    line_start(1, wl_ref.at[pl.ds(pl.multiple_of(core * half, half), half)], wl_at)
    line_start(2, we_ref, we_at)
    line_start(3, wo_ref, wo_at)
    owns = [
        pltpu.make_async_copy(wq_ref, wq_v.at[me], own_sem.at[0]),
        pltpu.make_async_copy(wl_ref.at[pl.ds(0, half)], wl_v.at[me, 0], own_sem.at[1]),
        pltpu.make_async_copy(wl_ref.at[pl.ds(half, half)], wl_v.at[me, 1], own_sem.at[2]),
        pltpu.make_async_copy(we_ref, we_v.at[me], own_sem.at[3]),
        pltpu.make_async_copy(wo_ref, wo_v.at[me], own_sem.at[4]),
    ]
    for copy in owns:
        copy.start()

    for j in range(n_t):
        for m in range(micros):
            x_v[j * share + m * chunk : j * share + (m + 1) * chunk] = saved_ref[
                m, j * chunk : (j + 1) * chunk
            ]
    for copy in owns:
        copy.wait()
    collect_dp(0, sm_v)
    gain = jnp.concatenate([sm_v[d][0:1, :wcol] for d in range(n)], axis=1)
    lgain = jnp.concatenate([sm_v[d][0:1, wcol : wcol + ccol] for d in range(n)], axis=1)
    x32 = x_v[...].astype(F32)
    r = lax.rsqrt(jnp.mean(x32 * x32, axis=1, keepdims=True) + EPS)
    nb = (x32 * r * gain).astype(BF)
    nb_v[...] = nb

    pair_copies = []

    def to_partner(block, valid, way, s):
        copy = rcopy(wl_v.at[block, core], wl_v.at[block, core], pair_s.at[block], pair_r.at[block], ten_dev(partner))
        begin(valid, copy)
        pair_copies.append((valid, block))

    def cols(b):
        return pl.ds(pl.multiple_of(b * wcol, wcol), wcol)

    def use_query(b):
        q_v[...] += mm(nb_v[:, cols(b)], wq_v[b])

    def use_latent(b):
        lat_v[...] += mm_nt(nb_v[:, cols(b)], wl_v[b].reshape(2 * half, wcol))

    last = sec == n_pipe - 1

    @pl.when(last)
    def _():
        for j in range(n_t):
            for m in range(micros):
                u_v[j, m * chunk : (m + 1) * chunk] = top_ref[m, j * chunk : (j + 1) * chunk]

    q_v[...] = mm(nb_v[:, cols(me)], wq_v[me])
    lat_v[...] = mm_nt(nb_v[:, cols(me)], wl_v[me].reshape(2 * half, wcol))

    def settle_latent(pairs):
        for valid, block in pairs:
            @pl.when(valid)
            def _(block=block):
                rcopy(
                    wl_v.at[block, 1 - core], wl_v.at[block, 1 - core], pair_s.at[block], pair_r.at[block], ten_dev(partner)
                ).wait_recv()
                use_latent(block)

    for s in range(n - 1):
        line_step(0, wq_at, s)
        line_step(1, wl_at, s, to_partner)
        for valid, block in pair_copies[-2:]:
            @pl.when(valid)
            def _(block=block):
                use_query(block)

        line_step(2, we_at, s)
        line_step(3, wo_at, s)
        settle_latent(pair_copies[-2:])

    wq = wq_v[...].reshape(width, wq_v.shape[2])
    wl = [wl_v[d].reshape(2 * half, wcol) for d in range(n)]
    we = we_v[...].reshape(n * ccol, we_v.shape[2])
    q = q_v[...]
    lat = lat_v[...]
    rank = n * ccol
    l32 = lat[:, :rank]
    rl = lax.rsqrt(jnp.mean(l32 * l32, axis=1, keepdims=True) + EPS)
    cb = (l32 * rl * lgain).astype(BF)
    cb_v[...] = cb
    spread_dp(1, lambda j: nb_v.at[:, pl.ds(j * wcol, wcol)], nc_v)
    spread_dp(2, lambda j: cb_v.at[:, pl.ds(j * ccol, ccol)], cc_v)
    ex = mm(cb, we)
    cosine, sine = cos_ref[...], sin_ref[...]
    lr = lat[:, rank:]
    lr2 = jnp.concatenate([lr, lr], axis=1)
    rk = (lr2 * cosine + half_swap(lr2) * sine).astype(BF)
    lane = lax.broadcasted_iota(jnp.int32, (rows, 2 * ROPE), 1)
    low = lane < ROPE
    q1, q2 = q[:, NOPE : 2 * NOPE], q[:, 2 * NOPE :]
    nope = (q[:, :NOPE], pltpu.roll(jnp.where(low, q2, q1), ROPE, 1))
    qr_all = jnp.where(low, q1, q2)
    qr = qr_all * cosine + half_swap(qr_all) * sine
    row = lax.broadcasted_iota(jnp.int32, (rows, rows), 0)
    col = lax.broadcasted_iota(jnp.int32, (rows, rows), 1)

    def place(i):
        return (i // share) * chunk + lax.rem(i, chunk)

    same = lax.rem(row, share) // chunk == lax.rem(col, share) // chunk
    keep = jnp.logical_and(same, place(row) >= place(col))
    scale = (NOPE + ROPE) ** (-0.5)
    heads = []
    for h in range(2):
        qn = nope[h].astype(BF)
        kn = ex[:, h * (NOPE + VDIM) : h * (NOPE + VDIM) + NOPE].astype(BF)
        vv = ex[:, h * (NOPE + VDIM) + NOPE : (h + 1) * (NOPE + VDIM)].astype(BF)
        mask = low if h == 0 else jnp.logical_not(low)
        qh = jnp.where(mask, qr, 0.0).astype(BF)
        scores = (mm_nt(qn, kn) + mm_nt(qh, rk)) * scale
        scores = jnp.where(keep, scores, -1e30)
        e = jnp.exp(scores - jnp.max(scores, axis=1, keepdims=True))
        w32 = e / jnp.sum(e, axis=1, keepdims=True)
        wb = w32.astype(BF)
        mx_v[me, :, h * VDIM : (h + 1) * VDIM] = mm(wb, vv).astype(BF)
        heads.append((qn, kn, vv, mask, qh, w32, wb))
    spread_dp(3, lambda j: mx_v.at[me], mx_v)
    for j in range(n):
        @pl.when(j == me)
        def _():
            nc_v[j] = nb_v[:, j * wcol : (j + 1) * wcol]
            cc_v[j] = cb_v[:, j * ccol : (j + 1) * ccol]

    for j in range(n_t):
        @pl.when(sec < n_pipe - 1)
        def _():
            rcopy(
                u_v.at[j], u_v.at[j], pipe_s.at[j], pipe_r.at[j], (jnp.minimum(sec + 1, n_pipe - 1), me, j)
            ).wait_recv()

    ub = u_v[...].reshape(rows, width)
    for j in range(n):
        uc_v[1, j] = ub[:, j * wcol : (j + 1) * wcol]
    spread_dp(4, lambda j: uc_v.at[1, j], uc_v.at[0])
    uc_v[0, me] = uc_v[1, me]
    dm = jnp.zeros((rows, wo_v.shape[1]), F32)
    for j in range(n):
        dm = dm + mm_nt(ub[:, j * wcol : (j + 1) * wcol], wo_v[j])
    dm = dm.astype(BF)
    dqr = jnp.zeros((rows, 2 * ROPE), F32)
    drk = jnp.zeros((rows, 2 * ROPE), F32)
    dqn = []
    for h, (qn, kn, vv, mask, qh, w32, wb) in enumerate(heads):
        dmh = dm[:, h * VDIM : (h + 1) * VDIM]
        dv = mm_tn(wb, dmh)
        dw = mm_nt(dmh, vv).astype(BF).astype(F32)
        ds = (w32 * (dw - jnp.sum(dw * w32, axis=1, keepdims=True)) * scale).astype(BF)
        dqn.append(mm(ds, kn))
        dqr = dqr + jnp.where(mask, mm(ds, rk), 0.0)
        drk = drk + mm_tn(ds, qh)
        de_v[me, :, h * (NOPE + VDIM) : h * (NOPE + VDIM) + NOPE] = mm_tn(ds, qn).astype(BF)
        de_v[me, :, h * (NOPE + VDIM) + NOPE : (h + 1) * (NOPE + VDIM)] = dv.astype(BF)
    dqr = dqr * cosine - half_swap(dqr) * sine
    turned = pltpu.roll(dqn[1], ROPE, 1)
    dq_v[me, :, :NOPE] = dqn[0].astype(BF)
    dq_v[me, :, NOPE : 2 * NOPE] = jnp.where(low, dqr, turned).astype(BF)
    dq_v[me, :, 2 * NOPE :] = jnp.where(low, turned, dqr).astype(BF)
    drk = drk * cosine - half_swap(drk) * sine
    drk = drk + pltpu.roll(drk, ROPE, 1)
    line_start(4, dq_v.at[me], dq_at)
    line_start(5, de_v.at[me], de_at)
    dc = mm_nt(de_v[me], we)
    dlg = jnp.sum(dc * l32 * rl, axis=0, keepdims=True)
    dcg = dc * lgain
    dl = rl * dcg - l32 * (rl * rl * rl) * jnp.mean(l32 * dcg, axis=1, keepdims=True)
    dlat = jnp.concatenate([dl.astype(BF), drk[:, :ROPE].astype(BF)], axis=1)
    dn = mm_nt(dq_v[me], wq) + jnp.concatenate([mm(dlat, wl[d]) for d in range(n)], axis=1)
    part_v[...] = dn.astype(BF).reshape(n_t, share, width)
    spread_ten(0, lambda j: part_v.at[j], rs_v)
    lp_v[...] = dlat.reshape(n_t, share, dlat.shape[1])
    spread_ten(3, lambda j: lp_v.at[j], ls_v)
    rs_v[ten] = part_v[ten]
    ls_v[ten] = lp_v[ten]
    bottom = sec == 0
    line_step(4, dq_at, 0, gate=bottom)
    line_step(5, de_at, 0, gate=bottom)
    collect_ten(0, rs_v)
    dns = jnp.sum(rs_v[...].astype(F32), axis=0)
    x_my = x_v[pl.ds(pl.multiple_of(ten * share, share), share)].astype(F32)
    r_my = lax.rsqrt(jnp.mean(x_my * x_my, axis=1, keepdims=True) + EPS)
    dng = dns * gain
    u_my = u_v[ten].astype(F32)
    dx = u_my + r_my * dng - x_my * (r_my * r_my * r_my) * jnp.mean(x_my * dng, axis=1, keepdims=True)
    dx_v[...] = dx.astype(BF)
    for j in range(n_t):
        begin(sec > 0, rcopy(dx_v, u_v.at[ten], pipe_s.at[j], pipe_r.at[ten], (jnp.maximum(sec - 1, 0), me, j)))
    collect_ten(3, ls_v)
    dl_v[ten, me] = jnp.sum(ls_v[...].astype(F32), axis=0).astype(BF)
    line_start(6, dl_v.at[ten, me], dl_at)
    dgain = jnp.sum(dns * x_my * r_my, axis=0, keepdims=True)
    for j in range(n):
        piece = jnp.concatenate(
            [dgain[:, j * wcol : (j + 1) * wcol], dlg[:, j * ccol : (j + 1) * ccol]], axis=1
        )
        sg_v[j] = jnp.broadcast_to(piece, sg_v.shape[1:])
    spread_dp(5, lambda j: sg_v.at[j], sr_v)
    sr_v[me] = sg_v[me]

    def to_tensor(block, valid=None, way=0, s=0):
        for j in range(n_t):
            cond = j != ten if valid is None else jnp.logical_and(valid, j != ten)
            begin(
                cond,
                rcopy(dl_v.at[ten, block], dl_v.at[ten, block], lat_s.at[j, block], lat_r.at[ten, block], ten_dev(j)),
            )

    to_tensor(me)
    line_step(4, dq_at, 0, gate=sec > 0)
    line_step(5, de_at, 0, gate=sec > 0)
    for m in range(micros):
        ig_ref[m] = dx[m * chunk : (m + 1) * chunk].astype(BF)
    for s in range(1, n - 1):
        line_step(6, dl_at, s - 1, to_tensor)
        line_step(4, dq_at, s)
        line_step(5, de_at, s)
    line_step(6, dl_at, n - 2, to_tensor)
    collect_dp(5, sr_v)
    st_v[ten] = jnp.sum(sr_v[...], axis=0)
    spread_ten(2, lambda j: st_v.at[ten], st_v)
    collect_dp(1, nc_v)
    collect_dp(2, cc_v)
    collect_dp(3, mx_v)
    collect_dp(4, uc_v.at[0])
    nc = nc_v[...].reshape(n * rows, wcol)
    gq_ref[...] = mm_tn(nc, dq_v[...].reshape(n * rows, dq_v.shape[2]))
    ge_ref[...] = mm_tn(cc_v[...].reshape(n * rows, ccol), de_v[...].reshape(n * rows, de_v.shape[2]))
    go_ref[...] = mm_tn(mx_v[...].reshape(n * rows, mx_v.shape[2]), uc_v[0].reshape(n * rows, wcol))
    for j in range(n_t):
        for d in range(n):
            @pl.when(j != ten)
            def _():
                rcopy(dl_v.at[j, d], dl_v.at[j, d], lat_s.at[j, d], lat_r.at[j, d], ten_dev(j)).wait_recv()

    acc = jnp.zeros(gl_ref.shape, F32)
    for d in range(n):
        block = jnp.concatenate([dl_v[j, d] for j in range(n_t)], axis=0)
        acc = acc + mm_tn(block, nc_v[d])
    gl_ref[...] = acc
    collect_ten(2, st_v)
    summed = jnp.sum(st_v[...], axis=0)
    gg_ref[...] = summed[0:1, :wcol]
    glg_ref[...] = summed[0:1, wcol:]
    for cond, copy in drains:
        @pl.when(cond)
        def _(copy=copy):
            copy.wait_send()


def section_step(saved, top_grad, gain, w_query, w_latent, compressed_gain, expand_weight, w_output):
    n_pipe, n, n_t = (lax.axis_size(a) for a in ("pipe", "dp", "tensor"))
    micros, seq, width = saved.shape[1:]
    wcol, ccol = gain.shape[1], compressed_gain.shape[1]
    rows, share = micros * seq, micros * seq // n_t
    qcols, lcols = w_query.shape[2], w_latent.shape[2]
    ecols, orows = expand_weight.shape[2], w_output.shape[1]
    order = np.arange(rows)
    place = (order // share) * (seq // n_t) + order % (seq // n_t)
    pair = np.arange(2 * ROPE) % (ROPE // 2)
    angle = place[:, None] * np.exp(-np.log(10000.0) * pair / (ROPE // 2))[None, :]
    sign = np.where(np.arange(2 * ROPE) % ROPE < ROPE // 2, -1.0, 1.0)
    cosine = jnp.asarray(np.cos(angle), F32)
    sine = jnp.asarray(np.sin(angle) * sign, F32)
    vm = pl.BlockSpec(memory_space=pltpu.VMEM)
    shape = jax.ShapeDtypeStruct
    dma = pltpu.SemaphoreType.DMA
    ig, gg, gq, gl, glg, ge, go = pl.pallas_call(
        lambda *refs: section_kernel((n_pipe, n, n_t, micros, seq), *refs),
        name="section_step",
        out_shape=(
            shape((micros, seq // n_t, width), BF),
            shape((1, wcol), F32),
            shape((wcol, qcols), F32),
            shape((lcols, wcol), F32),
            shape((1, ccol), F32),
            shape((ccol, ecols), F32),
            shape((orows, wcol), F32),
        ),
        in_specs=[vm] * 10,
        out_specs=(vm,) * 7,
        scratch_shapes=[
            pltpu.VMEM((rows, width), BF),
            pltpu.VMEM((8, wcol + ccol), F32),
            pltpu.VMEM((n_t, share, width), BF),
            pltpu.VMEM((rows, width), BF),
            pltpu.VMEM((rows, n * ccol), BF),
            pltpu.VMEM((n, 8, wcol + ccol), F32),
            pltpu.VMEM((n, wcol, qcols), BF),
            pltpu.VMEM((n, 2, lcols // 2, wcol), BF),
            pltpu.VMEM((n, ccol, ecols), BF),
            pltpu.VMEM((n, orows, wcol), BF),
            pltpu.VMEM((n, rows, wcol), BF),
            pltpu.VMEM((n, rows, ccol), BF),
            pltpu.VMEM((n, rows, orows), BF),
            pltpu.VMEM((2, n, rows, wcol), BF),
            pltpu.VMEM((n, rows, qcols), BF),
            pltpu.VMEM((n, rows, ecols), BF),
            pltpu.VMEM((n_t, n, share, lcols), BF),
            pltpu.VMEM((n_t, share, width), BF),
            pltpu.VMEM((n_t, share, width), BF),
            pltpu.VMEM((n_t, share, lcols), BF),
            pltpu.VMEM((n_t, share, lcols), BF),
            pltpu.VMEM((rows, qcols), F32),
            pltpu.VMEM((rows, lcols), F32),
            pltpu.VMEM((share, width), BF),
            pltpu.VMEM((n, 8, wcol + ccol), F32),
            pltpu.VMEM((n, 8, wcol + ccol), F32),
            pltpu.VMEM((n_t, 8, wcol + ccol), F32),
            dma((6,)),
            dma((7, 2, n)),
            dma((7, n)),
            dma((n,)),
            dma((n,)),
            dma((6, n)),
            dma((6, n)),
            dma((4, n_t)),
            dma((4, n_t)),
            dma((n_t,)),
            dma((n_t,)),
            dma((n_t, n)),
            dma((n_t, n)),
        ],
        compiler_params=pltpu.CompilerParams(
            collective_id=0, has_side_effects=True, vmem_limit_bytes=60 * 1024 * 1024
        ),
    )(
        saved[0], top_grad, gain, compressed_gain, w_query[0], w_latent[0].T,
        expand_weight[0], w_output[0], cosine, sine,
    )
    return ig[None], gg, gq[None], gl.T[None], glg, ge[None], go[None]


def choose(saved, top_grad, gain, w_query, w_latent, compressed_gain, expand_weight, w_output):
    arrays = (saved, top_grad, gain, w_query, w_latent, compressed_gain, expand_weight, w_output)
    n_t = lax.axis_size("tensor")
    fits = (
        lax.axis_size("dp") > 1
        and n_t % 2 == 0
        and w_query.shape[2] == 2 * (NOPE + ROPE)
        and gain.shape[1] % 128 == 0
        and compressed_gain.shape[1] % 128 == 0
        and saved.shape[2] % (16 * n_t) == 0
    )
    return section_step(*arrays) if fits else shards(*arrays)


def solution(mesh):
    in_specs = (
        P("pipe", None, "dp", None),
        P(None, "dp", None),
        P("pipe", "dp"),
        P("pipe", "dp", "tensor"),
        P("pipe", "dp", None),
        P("pipe", "dp"),
        P("pipe", "dp", "tensor"),
        P("pipe", "tensor", "dp"),
    )
    out_specs = (
        P("pipe", None, ("dp", "tensor"), None),
        P("pipe", "dp"),
        P("pipe", "dp", "tensor"),
        P("pipe", "dp", None),
        P("pipe", "dp"),
        P("pipe", "dp", "tensor"),
        P("pipe", "tensor", "dp"),
    )
    return jax.shard_map(choose, mesh=mesh, in_specs=in_specs, out_specs=out_specs, check_vma=False)
```

```python
import jax
import jax.numpy as jnp
from jax import lax
import numpy as np
from jax.experimental import pallas as pl
from jax.experimental.pallas import tpu as pltpu
from jax.sharding import PartitionSpec as P

NOPE = 128
ROPE = 64
VDIM = 128
COMPRESSED_RANK = 512


EPS = 1e-06


def passed_along(value, axis, steps):
    count = lax.axis_size(axis)
    first, last = (max(0, -steps), min(count, count - steps))
    return lax.ppermute(value, axis, [(source, source + steps) for source in range(first, last)])


def root_mean_scale(values, scale):
    return values * lax.rsqrt(jnp.mean(values * values, axis=-1, keepdims=True) + EPS) * scale


def rotary_angles(values):
    length = values.shape[0]
    half = values.shape[-1] // 2
    freq = jnp.exp(-jnp.log(10000.0) * jnp.arange(half, dtype=jnp.float32) / half)
    angle = jnp.arange(length, dtype=jnp.float32)[:, None] * freq[None, :]
    cosine = jnp.cos(angle)[:, None, :]
    sine = jnp.sin(angle)[:, None, :]
    first = values[..., :half]
    second = values[..., half:]
    return jnp.concatenate(
        [first * cosine - second * sine, second * cosine + first * sine], axis=-1
    )


def branch(normed, w_q, w_lat, latent_norm_gain, w_exp, w_out):
    length = normed.shape[0]
    heads = w_q.shape[1] // (NOPE + ROPE)
    rounded = normed.astype(jnp.bfloat16)
    query = jnp.dot(rounded, w_q, preferred_element_type=jnp.float32).reshape(
        length, heads, NOPE + ROPE
    )
    latent_state = jnp.dot(rounded, w_lat, preferred_element_type=jnp.float32)
    compressed_state = root_mean_scale(latent_state[:, :COMPRESSED_RANK], latent_norm_gain).astype(
        jnp.bfloat16
    )
    rotary_key_part = rotary_angles(latent_state[:, None, COMPRESSED_RANK:])[:, 0, :]
    expanded = jnp.dot(compressed_state, w_exp, preferred_element_type=jnp.float32).reshape(
        length, heads, NOPE + VDIM
    )
    key_nope = expanded[:, :, :NOPE]
    values = expanded[:, :, NOPE:].astype(jnp.bfloat16)
    query_rope = rotary_angles(query[:, :, NOPE:])
    scores = jnp.einsum("qhd,khd->hqk", query[:, :, :NOPE], key_nope) + jnp.einsum(
        "qhd,kd->hqk", query_rope, rotary_key_part
    )
    scores = scores * (NOPE + ROPE) ** (-0.5)
    causal = jnp.arange(length)[:, None] >= jnp.arange(length)[None, :]
    scores = jnp.where(causal[None], scores, -1e30)
    weights = jax.nn.softmax(scores, axis=-1).astype(jnp.bfloat16)
    mixed = jnp.einsum("hqk,khd->qhd", weights.astype(jnp.float32), values.astype(jnp.float32))
    mixed = mixed.astype(jnp.bfloat16).reshape(length, heads * VDIM)
    return jnp.dot(mixed, w_out, preferred_element_type=jnp.float32)


def shards(saved, top_grad, gain, w_query, w_latent, compressed_gain, expand_weight, w_output):
    gathered = (
        lax.all_gather(gain, "dp", axis=1, tiled=True),
        lax.all_gather(w_query, "dp", axis=1, tiled=True),
        lax.all_gather(w_latent, "dp", axis=1, tiled=True),
        lax.all_gather(compressed_gain, "dp", axis=1, tiled=True),
        lax.all_gather(expand_weight, "dp", axis=1, tiled=True),
        lax.all_gather(w_output, "dp", axis=2, tiled=True),
    )
    gain32 = gathered[0][0].astype(jnp.float32)
    query_all = gathered[1][0]
    latent_all = gathered[2][0]
    lgain32 = gathered[3][0].astype(jnp.float32)
    expand_all = gathered[4][0]
    output_all = gathered[5][0]
    sections = lax.axis_size("pipe")
    section_index = lax.axis_index("pipe")
    tensor_count = lax.axis_size("tensor")
    tensor_rank = lax.axis_index("tensor")
    micro_count = saved.shape[1]
    length = saved.shape[2]
    width = saved.shape[3]
    share = length // tensor_count

    def compute(normed, upstream):
        unused, pull = jax.vjp(
            lambda value: branch(value, query_all, latent_all, lgain32, expand_all, output_all),
            normed,
        )
        return pull(upstream.astype(jnp.float32))[0]

    def skip(normed, upstream):
        return jnp.zeros_like(normed)

    gain_total = jnp.zeros((width,), jnp.float32)
    results = jnp.zeros((micro_count, share, width), jnp.bfloat16)
    stored = jnp.zeros((micro_count, length, width), jnp.bfloat16)
    received = jnp.zeros((length, width), jnp.bfloat16)
    for tick in range(sections + micro_count - 1):
        micro = tick - (sections - 1 - section_index)
        active = jnp.logical_and(micro >= 0, micro < micro_count)
        picked = jnp.clip(micro, 0, micro_count - 1)
        x_rows = lax.dynamic_index_in_dim(saved[0], picked, 0, keepdims=False)
        top_rows = lax.dynamic_index_in_dim(top_grad, picked, 0, keepdims=False)
        arrived = received
        upstream = jnp.where(section_index == sections - 1, top_rows, arrived)
        x_float = x_rows.astype(jnp.float32)
        normed, norm_pull = jax.vjp(root_mean_scale, x_float, gain32)
        branch_grad = lax.cond(active, compute, skip, normed, upstream)
        d_normed = lax.psum(branch_grad.astype(jnp.bfloat16), "tensor").astype(jnp.float32)
        dx_norm, d_gain = norm_pull(d_normed)
        dx = (upstream.astype(jnp.float32) + dx_norm).astype(jnp.bfloat16)
        gain_total = gain_total + jnp.where(active, d_gain, 0.0)
        mine = lax.dynamic_slice_in_dim(dx, tensor_rank * share, share, 0)
        chosen = (jnp.arange(micro_count) == micro)[:, None, None]
        results = jnp.where(chosen, mine[None], results)
        stored = jnp.where(chosen, upstream[None], stored)
        received = passed_along(dx, "pipe", -1)
    totals = (
        jnp.zeros(query_all.shape, jnp.float32),
        jnp.zeros(latent_all.shape, jnp.float32),
        jnp.zeros(lgain32.shape, jnp.float32),
        jnp.zeros(expand_all.shape, jnp.float32),
        jnp.zeros(output_all.shape, jnp.float32),
    )
    for micro_index in range(micro_count):
        normed_again = root_mean_scale(saved[0, micro_index].astype(jnp.float32), gain32)
        unused, weight_pull = jax.vjp(
            lambda w_q, w_lat, lat_gain, w_exp, w_out: branch(
                normed_again, w_q, w_lat, lat_gain, w_exp, w_out
            ),
            query_all,
            latent_all,
            lgain32,
            expand_all,
            output_all,
        )
        cotangents = weight_pull(stored[micro_index].astype(jnp.float32))
        totals = tuple(
            (total + piece.astype(jnp.float32) for total, piece in zip(totals, cotangents))
        )
    gain_part = jnp.where(tensor_rank == 0, gain_total, 0.0)
    grad_q, grad_lat, grad_lg, grad_e, grad_o = totals
    out_q, part_lat, part_lg, out_e, out_o, part_gain = (
        lax.psum_scatter(grad_q.astype(jnp.bfloat16), "dp", scatter_dimension=0, tiled=True).astype(
            jnp.float32
        ),
        lax.psum_scatter(
            grad_lat.astype(jnp.bfloat16), "dp", scatter_dimension=0, tiled=True
        ).astype(jnp.float32),
        lax.psum_scatter(
            grad_lg.astype(jnp.bfloat16), "dp", scatter_dimension=0, tiled=True
        ).astype(jnp.float32),
        lax.psum_scatter(grad_e.astype(jnp.bfloat16), "dp", scatter_dimension=0, tiled=True).astype(
            jnp.float32
        ),
        lax.psum_scatter(grad_o.astype(jnp.bfloat16), "dp", scatter_dimension=1, tiled=True).astype(
            jnp.float32
        ),
        lax.psum_scatter(
            gain_part.astype(jnp.bfloat16), "dp", scatter_dimension=0, tiled=True
        ).astype(jnp.float32),
    )
    out_lat, out_lg, out_gain = (
        lax.psum(part_lat.astype(jnp.bfloat16), "tensor").astype(jnp.float32),
        lax.psum(part_lg.astype(jnp.bfloat16), "tensor").astype(jnp.float32),
        lax.psum(part_gain.astype(jnp.bfloat16), "tensor").astype(jnp.float32),
    )
    return (
        results[None],
        out_gain[None],
        out_q[None],
        out_lat[None],
        out_lg[None],
        out_e[None],
        out_o[None],
    )


MESH = pl.DeviceIdType.MESH
BF = jnp.bfloat16
F32 = jnp.float32


def mm(a, b):
    return lax.dot_general(a, b, (((1,), (0,)), ((), ())), preferred_element_type=F32)


def mm_nt(a, b):
    return lax.dot_general(a, b, (((1,), (1,)), ((), ())), preferred_element_type=F32)


def mm_tn(a, b):
    return lax.dot_general(a, b, (((0,), (0,)), ((), ())), preferred_element_type=F32)


def half_swap(v):
    lane = lax.broadcasted_iota(jnp.int32, v.shape, 1)
    ahead = pltpu.roll(v, v.shape[1] - ROPE // 2, 1)
    behind = pltpu.roll(v, ROPE // 2, 1)
    return jnp.where(lax.rem(lane, ROPE) < ROPE // 2, ahead, behind)


def section_kernel(
    dims,
    saved_ref, top_ref, gain_ref, lgain_ref, wq_ref, wl_ref, we_ref, wo_ref, cos_ref, sin_ref,
    ig_ref, gg_ref, gq_ref, gl_ref, glg_ref, ge_ref, go_ref,
    x_v, own_v, u_v, nb_v, cb_v, sm_v, wq_v, wl_v, we_v, wo_v,
    nc_v, cc_v, mx_v, uc_v, dq_v, de_v, dl_v, part_v, rs_v, lp_v, ls_v, q_v, lat_v, dx_v, sg_v, sr_v, st_v,
    own_sem, line_s, line_r, pair_s, pair_r, dp_s, dp_r, ten_s, ten_r, pipe_s, pipe_r, lat_s, lat_r,
):
    n_pipe, n, n_t, micros, seq = dims
    sec, me, ten = lax.axis_index("pipe"), lax.axis_index("dp"), lax.axis_index("tensor")
    rows = micros * seq
    chunk = seq // n_t
    share = micros * chunk
    width = x_v.shape[1]
    wcol = wq_v.shape[1]
    ccol = we_v.shape[1]
    core = lax.rem(ten, 2)
    partner = ten + 1 - 2 * core
    half = wl_ref.shape[0] // 2
    drains = []

    def rcopy(a, b, ss, rs, dev):
        return pltpu.make_async_remote_copy(
            src_ref=a, dst_ref=b, send_sem=ss, recv_sem=rs, device_id=dev, device_id_type=MESH
        )

    def begin(cond, copy):
        @pl.when(cond)
        def _():
            copy.start()

        drains.append((cond, copy))

    def dp_dev(d):
        return (sec, d, ten)

    def ten_dev(d):
        return (sec, me, d)

    barrier = pltpu.get_barrier_semaphore()
    for j in range(n):
        @pl.when(j != me)
        def _():
            pl.semaphore_signal(barrier, inc=1, device_id=dp_dev(j), device_id_type=MESH)

    for j in range(n_t):
        @pl.when(j != ten)
        def _():
            pl.semaphore_signal(barrier, inc=1, device_id=ten_dev(j), device_id_type=MESH)

        @pl.when(sec > 0)
        def _():
            pl.semaphore_signal(barrier, inc=1, device_id=(sec - 1, me, j), device_id_type=MESH)

        @pl.when(sec < n_pipe - 1)
        def _():
            pl.semaphore_signal(barrier, inc=1, device_id=(sec + 1, me, j), device_id_type=MESH)

    neighbours = jnp.minimum(sec, 1) + jnp.minimum(n_pipe - 1 - sec, 1)
    pl.semaphore_wait(barrier, n - 1 + n_t - 1 + neighbours * n_t)

    def line_start(k, source, at):
        begin(me < n - 1, rcopy(source, at(me), line_s.at[k, 0, 0], line_r.at[k, me], dp_dev(me + 1)))
        begin(me > 0, rcopy(source, at(me), line_s.at[k, 1, 0], line_r.at[k, me], dp_dev(me - 1)))

    def line_step(k, at, s, extra=None, gate=None):
        for way, block, valid, more, dest in (
            (0, jnp.maximum(me - 1 - s, 0), me - 1 - s >= 0, me < n - 1, me + 1),
            (1, jnp.minimum(me + 1 + s, n - 1), me + 1 + s <= n - 1, me > 0, me - 1),
        ):
            if gate is not None:
                valid = jnp.logical_and(valid, gate)
            arrived = rcopy(at(block), at(block), line_s.at[k, way, s + 1], line_r.at[k, block], dp_dev(dest))

            @pl.when(valid)
            def _():
                arrived.wait_recv()

            if s < n - 2:
                begin(jnp.logical_and(valid, more), arrived)
            if extra is not None:
                extra(block, valid, way, s)

    def spread_dp(k, source, dest):
        for j in range(n):
            begin(j != me, rcopy(source(j), dest.at[me], dp_s.at[k, j], dp_r.at[k, me], dp_dev(j)))

    def collect_dp(k, dest):
        for j in range(n):
            @pl.when(j != me)
            def _():
                rcopy(dest.at[j], dest.at[j], dp_s.at[k, j], dp_r.at[k, j], dp_dev(j)).wait_recv()

    def spread_ten(k, source, dest):
        for j in range(n_t):
            begin(j != ten, rcopy(source(j), dest.at[ten], ten_s.at[k, j], ten_r.at[k, ten], ten_dev(j)))

    def collect_ten(k, dest):
        for j in range(n_t):
            @pl.when(j != ten)
            def _():
                rcopy(dest.at[j], dest.at[j], ten_s.at[k, j], ten_r.at[k, j], ten_dev(j)).wait_recv()

    wq_at = lambda b: wq_v.at[b]
    wl_at = lambda b: wl_v.at[b, core]
    we_at = lambda b: we_v.at[b]
    wo_at = lambda b: wo_v.at[b]
    dq_at = lambda b: dq_v.at[b]
    de_at = lambda b: de_v.at[b]
    dl_at = lambda b: dl_v.at[ten, b]

    own_v[:, :wcol] = jnp.broadcast_to(gain_ref[...].astype(F32), (8, wcol))
    own_v[:, wcol:] = jnp.broadcast_to(lgain_ref[...].astype(F32), (8, ccol))
    spread_dp(0, lambda j: own_v, sm_v)
    sm_v[me] = own_v[...]
    line_start(0, wq_ref, wq_at)
    line_start(1, wl_ref.at[pl.ds(pl.multiple_of(core * half, half), half)], wl_at)
    line_start(2, we_ref, we_at)
    line_start(3, wo_ref, wo_at)
    owns = [
        pltpu.make_async_copy(wq_ref, wq_v.at[me], own_sem.at[0]),
        pltpu.make_async_copy(wl_ref.at[pl.ds(0, half)], wl_v.at[me, 0], own_sem.at[1]),
        pltpu.make_async_copy(wl_ref.at[pl.ds(half, half)], wl_v.at[me, 1], own_sem.at[2]),
        pltpu.make_async_copy(we_ref, we_v.at[me], own_sem.at[3]),
        pltpu.make_async_copy(wo_ref, wo_v.at[me], own_sem.at[4]),
    ]
    for copy in owns:
        copy.start()

    for j in range(n_t):
        for m in range(micros):
            x_v[j * share + m * chunk : j * share + (m + 1) * chunk] = saved_ref[
                m, j * chunk : (j + 1) * chunk
            ]
    for copy in owns:
        copy.wait()
    collect_dp(0, sm_v)
    gain = jnp.concatenate([sm_v[d][0:1, :wcol] for d in range(n)], axis=1)
    lgain = jnp.concatenate([sm_v[d][0:1, wcol : wcol + ccol] for d in range(n)], axis=1)
    x32 = x_v[...].astype(F32)
    r = lax.rsqrt(jnp.mean(x32 * x32, axis=1, keepdims=True) + EPS)
    nb = (x32 * r * gain).astype(BF)
    nb_v[...] = nb

    pair_copies = []

    def to_partner(block, valid, way, s):
        copy = rcopy(wl_v.at[block, core], wl_v.at[block, core], pair_s.at[block], pair_r.at[block], ten_dev(partner))
        begin(valid, copy)
        pair_copies.append((valid, block))

    def cols(b):
        return pl.ds(pl.multiple_of(b * wcol, wcol), wcol)

    def use_query(b):
        q_v[...] += mm(nb_v[:, cols(b)], wq_v[b])

    def use_latent(b):
        lat_v[...] += mm_nt(nb_v[:, cols(b)], wl_v[b].reshape(2 * half, wcol))

    last = sec == n_pipe - 1

    @pl.when(last)
    def _():
        for j in range(n_t):
            for m in range(micros):
                u_v[j, m * chunk : (m + 1) * chunk] = top_ref[m, j * chunk : (j + 1) * chunk]

    q_v[...] = mm(nb_v[:, cols(me)], wq_v[me])
    lat_v[...] = mm_nt(nb_v[:, cols(me)], wl_v[me].reshape(2 * half, wcol))

    def settle_latent(pairs):
        for valid, block in pairs:
            @pl.when(valid)
            def _(block=block):
                rcopy(
                    wl_v.at[block, 1 - core], wl_v.at[block, 1 - core], pair_s.at[block], pair_r.at[block], ten_dev(partner)
                ).wait_recv()
                use_latent(block)

    for s in range(n - 1):
        line_step(0, wq_at, s)
        line_step(1, wl_at, s, to_partner)
        for valid, block in pair_copies[-2:]:
            @pl.when(valid)
            def _(block=block):
                use_query(block)

        line_step(2, we_at, s)
        line_step(3, wo_at, s)
        settle_latent(pair_copies[-2:])

    wq = wq_v[...].reshape(width, wq_v.shape[2])
    wl = [wl_v[d].reshape(2 * half, wcol) for d in range(n)]
    we = we_v[...].reshape(n * ccol, we_v.shape[2])
    q = q_v[...]
    lat = lat_v[...]
    rank = n * ccol
    l32 = lat[:, :rank]
    rl = lax.rsqrt(jnp.mean(l32 * l32, axis=1, keepdims=True) + EPS)
    cb = (l32 * rl * lgain).astype(BF)
    cb_v[...] = cb
    spread_dp(1, lambda j: nb_v.at[:, pl.ds(j * wcol, wcol)], nc_v)
    spread_dp(2, lambda j: cb_v.at[:, pl.ds(j * ccol, ccol)], cc_v)
    ex = mm(cb, we)
    cosine, sine = cos_ref[...], sin_ref[...]
    lr = lat[:, rank:]
    lr2 = jnp.concatenate([lr, lr], axis=1)
    rk = (lr2 * cosine + half_swap(lr2) * sine).astype(BF)
    lane = lax.broadcasted_iota(jnp.int32, (rows, 2 * ROPE), 1)
    low = lane < ROPE
    q1, q2 = q[:, NOPE : 2 * NOPE], q[:, 2 * NOPE :]
    nope = (q[:, :NOPE], pltpu.roll(jnp.where(low, q2, q1), ROPE, 1))
    qr_all = jnp.where(low, q1, q2)
    qr = qr_all * cosine + half_swap(qr_all) * sine
    row = lax.broadcasted_iota(jnp.int32, (rows, rows), 0)
    col = lax.broadcasted_iota(jnp.int32, (rows, rows), 1)

    def place(i):
        return (i // share) * chunk + lax.rem(i, chunk)

    same = lax.rem(row, share) // chunk == lax.rem(col, share) // chunk
    keep = jnp.logical_and(same, place(row) >= place(col))
    scale = (NOPE + ROPE) ** (-0.5)
    heads = []
    for h in range(2):
        qn = nope[h].astype(BF)
        kn = ex[:, h * (NOPE + VDIM) : h * (NOPE + VDIM) + NOPE].astype(BF)
        vv = ex[:, h * (NOPE + VDIM) + NOPE : (h + 1) * (NOPE + VDIM)].astype(BF)
        mask = low if h == 0 else jnp.logical_not(low)
        qh = jnp.where(mask, qr, 0.0).astype(BF)
        scores = (mm_nt(qn, kn) + mm_nt(qh, rk)) * scale
        scores = jnp.where(keep, scores, -1e30)
        e = jnp.exp(scores - jnp.max(scores, axis=1, keepdims=True))
        w32 = e / jnp.sum(e, axis=1, keepdims=True)
        wb = w32.astype(BF)
        mx_v[me, :, h * VDIM : (h + 1) * VDIM] = mm(wb, vv).astype(BF)
        heads.append((qn, kn, vv, mask, qh, w32, wb))
    spread_dp(3, lambda j: mx_v.at[me], mx_v)
    for j in range(n):
        @pl.when(j == me)
        def _():
            nc_v[j] = nb_v[:, j * wcol : (j + 1) * wcol]
            cc_v[j] = cb_v[:, j * ccol : (j + 1) * ccol]

    for j in range(n_t):
        @pl.when(sec < n_pipe - 1)
        def _():
            rcopy(
                u_v.at[j], u_v.at[j], pipe_s.at[j], pipe_r.at[j], (jnp.minimum(sec + 1, n_pipe - 1), me, j)
            ).wait_recv()

    ub = u_v[...].reshape(rows, width)
    for j in range(n):
        uc_v[1, j] = ub[:, j * wcol : (j + 1) * wcol]
    spread_dp(4, lambda j: uc_v.at[1, j], uc_v.at[0])
    uc_v[0, me] = uc_v[1, me]
    dm = jnp.zeros((rows, wo_v.shape[1]), F32)
    for j in range(n):
        dm = dm + mm_nt(ub[:, j * wcol : (j + 1) * wcol], wo_v[j])
    dm = dm.astype(BF)
    dqr = jnp.zeros((rows, 2 * ROPE), F32)
    drk = jnp.zeros((rows, 2 * ROPE), F32)
    dqn = []
    for h, (qn, kn, vv, mask, qh, w32, wb) in enumerate(heads):
        dmh = dm[:, h * VDIM : (h + 1) * VDIM]
        dv = mm_tn(wb, dmh)
        dw = mm_nt(dmh, vv).astype(BF).astype(F32)
        ds = (w32 * (dw - jnp.sum(dw * w32, axis=1, keepdims=True)) * scale).astype(BF)
        dqn.append(mm(ds, kn))
        dqr = dqr + jnp.where(mask, mm(ds, rk), 0.0)
        drk = drk + mm_tn(ds, qh)
        de_v[me, :, h * (NOPE + VDIM) : h * (NOPE + VDIM) + NOPE] = mm_tn(ds, qn).astype(BF)
        de_v[me, :, h * (NOPE + VDIM) + NOPE : (h + 1) * (NOPE + VDIM)] = dv.astype(BF)
    dqr = dqr * cosine - half_swap(dqr) * sine
    turned = pltpu.roll(dqn[1], ROPE, 1)
    dq_v[me, :, :NOPE] = dqn[0].astype(BF)
    dq_v[me, :, NOPE : 2 * NOPE] = jnp.where(low, dqr, turned).astype(BF)
    dq_v[me, :, 2 * NOPE :] = jnp.where(low, turned, dqr).astype(BF)
    drk = drk * cosine - half_swap(drk) * sine
    drk = drk + pltpu.roll(drk, ROPE, 1)
    line_start(4, dq_v.at[me], dq_at)
    line_start(5, de_v.at[me], de_at)
    dc = mm_nt(de_v[me], we)
    dlg = jnp.sum(dc * l32 * rl, axis=0, keepdims=True)
    dcg = dc * lgain
    dl = rl * dcg - l32 * (rl * rl * rl) * jnp.mean(l32 * dcg, axis=1, keepdims=True)
    dlat = jnp.concatenate([dl.astype(BF), drk[:, :ROPE].astype(BF)], axis=1)
    dn = mm_nt(dq_v[me], wq) + jnp.concatenate([mm(dlat, wl[d]) for d in range(n)], axis=1)
    part_v[...] = dn.astype(BF).reshape(n_t, share, width)
    spread_ten(0, lambda j: part_v.at[j], rs_v)
    lp_v[...] = dlat.reshape(n_t, share, dlat.shape[1])
    spread_ten(3, lambda j: lp_v.at[j], ls_v)
    rs_v[ten] = part_v[ten]
    ls_v[ten] = lp_v[ten]
    bottom = sec == 0
    line_step(4, dq_at, 0, gate=bottom)
    line_step(5, de_at, 0, gate=bottom)
    collect_ten(0, rs_v)
    dns = jnp.sum(rs_v[...].astype(F32), axis=0)
    x_my = x_v[pl.ds(pl.multiple_of(ten * share, share), share)].astype(F32)
    r_my = lax.rsqrt(jnp.mean(x_my * x_my, axis=1, keepdims=True) + EPS)
    dng = dns * gain
    u_my = u_v[ten].astype(F32)
    dx = u_my + r_my * dng - x_my * (r_my * r_my * r_my) * jnp.mean(x_my * dng, axis=1, keepdims=True)
    dx_v[...] = dx.astype(BF)
    for j in range(n_t):
        begin(sec > 0, rcopy(dx_v, u_v.at[ten], pipe_s.at[j], pipe_r.at[ten], (jnp.maximum(sec - 1, 0), me, j)))
    collect_ten(3, ls_v)
    dl_v[ten, me] = jnp.sum(ls_v[...].astype(F32), axis=0).astype(BF)
    line_start(6, dl_v.at[ten, me], dl_at)
    dgain = jnp.sum(dns * x_my * r_my, axis=0, keepdims=True)
    for j in range(n):
        piece = jnp.concatenate(
            [dgain[:, j * wcol : (j + 1) * wcol], dlg[:, j * ccol : (j + 1) * ccol]], axis=1
        )
        sg_v[j] = jnp.broadcast_to(piece, sg_v.shape[1:])
    spread_dp(5, lambda j: sg_v.at[j], sr_v)
    sr_v[me] = sg_v[me]

    def to_tensor(block, valid=None, way=0, s=0):
        for j in range(n_t):
            cond = j != ten if valid is None else jnp.logical_and(valid, j != ten)
            begin(
                cond,
                rcopy(dl_v.at[ten, block], dl_v.at[ten, block], lat_s.at[j, block], lat_r.at[ten, block], ten_dev(j)),
            )

    to_tensor(me)
    line_step(4, dq_at, 0, gate=sec > 0)
    line_step(5, de_at, 0, gate=sec > 0)
    for m in range(micros):
        ig_ref[m] = dx[m * chunk : (m + 1) * chunk].astype(BF)
    for s in range(1, n - 1):
        line_step(6, dl_at, s - 1, to_tensor)
        line_step(4, dq_at, s)
        line_step(5, de_at, s)
    line_step(6, dl_at, n - 2, to_tensor)
    collect_dp(5, sr_v)
    st_v[ten] = jnp.sum(sr_v[...], axis=0)
    spread_ten(2, lambda j: st_v.at[ten], st_v)
    collect_dp(1, nc_v)
    collect_dp(2, cc_v)
    collect_dp(3, mx_v)
    collect_dp(4, uc_v.at[0])
    nc = nc_v[...].reshape(n * rows, wcol)
    gq_ref[...] = mm_tn(nc, dq_v[...].reshape(n * rows, dq_v.shape[2]))
    ge_ref[...] = mm_tn(cc_v[...].reshape(n * rows, ccol), de_v[...].reshape(n * rows, de_v.shape[2]))
    go_ref[...] = mm_tn(mx_v[...].reshape(n * rows, mx_v.shape[2]), uc_v[0].reshape(n * rows, wcol))
    for j in range(n_t):
        for d in range(n):
            @pl.when(j != ten)
            def _():
                rcopy(dl_v.at[j, d], dl_v.at[j, d], lat_s.at[j, d], lat_r.at[j, d], ten_dev(j)).wait_recv()

    acc = jnp.zeros(gl_ref.shape, F32)
    for d in range(n):
        block = jnp.concatenate([dl_v[j, d] for j in range(n_t)], axis=0)
        acc = acc + mm_tn(block, nc_v[d])
    gl_ref[...] = acc
    collect_ten(2, st_v)
    summed = jnp.sum(st_v[...], axis=0)
    gg_ref[...] = summed[0:1, :wcol]
    glg_ref[...] = summed[0:1, wcol:]
    for cond, copy in drains:
        @pl.when(cond)
        def _(copy=copy):
            copy.wait_send()


def hand_over(*refs):
    for source, dest in zip(refs[:7], refs[7:]):
        dest[...] = source[...]


def section_step(saved, top_grad, gain, w_query, w_latent, compressed_gain, expand_weight, w_output):
    n_pipe, n, n_t = (lax.axis_size(a) for a in ("pipe", "dp", "tensor"))
    micros, seq, width = saved.shape[1:]
    wcol, ccol = gain.shape[1], compressed_gain.shape[1]
    rows, share = micros * seq, micros * seq // n_t
    qcols, lcols = w_query.shape[2], w_latent.shape[2]
    ecols, orows = expand_weight.shape[2], w_output.shape[1]
    order = np.arange(rows)
    place = (order // share) * (seq // n_t) + order % (seq // n_t)
    pair = np.arange(2 * ROPE) % (ROPE // 2)
    angle = place[:, None] * np.exp(-np.log(10000.0) * pair / (ROPE // 2))[None, :]
    sign = np.where(np.arange(2 * ROPE) % ROPE < ROPE // 2, -1.0, 1.0)
    cosine = jnp.asarray(np.cos(angle), F32)
    sine = jnp.asarray(np.sin(angle) * sign, F32)
    vm = pl.BlockSpec(memory_space=pltpu.VMEM)
    shape = jax.ShapeDtypeStruct
    dma = pltpu.SemaphoreType.DMA
    ig, gg, gq, gl, glg, ge, go = pl.pallas_call(
        lambda *refs: section_kernel((n_pipe, n, n_t, micros, seq), *refs),
        name="section_step",
        out_shape=(
            shape((micros, seq // n_t, width), BF),
            shape((1, wcol), F32),
            shape((wcol, qcols), F32),
            shape((lcols, wcol), F32),
            shape((1, ccol), F32),
            shape((ccol, ecols), F32),
            shape((orows, wcol), F32),
        ),
        in_specs=[vm] * 10,
        out_specs=(vm,) * 7,
        scratch_shapes=[
            pltpu.VMEM((rows, width), BF),
            pltpu.VMEM((8, wcol + ccol), F32),
            pltpu.VMEM((n_t, share, width), BF),
            pltpu.VMEM((rows, width), BF),
            pltpu.VMEM((rows, n * ccol), BF),
            pltpu.VMEM((n, 8, wcol + ccol), F32),
            pltpu.VMEM((n, wcol, qcols), BF),
            pltpu.VMEM((n, 2, lcols // 2, wcol), BF),
            pltpu.VMEM((n, ccol, ecols), BF),
            pltpu.VMEM((n, orows, wcol), BF),
            pltpu.VMEM((n, rows, wcol), BF),
            pltpu.VMEM((n, rows, ccol), BF),
            pltpu.VMEM((n, rows, orows), BF),
            pltpu.VMEM((2, n, rows, wcol), BF),
            pltpu.VMEM((n, rows, qcols), BF),
            pltpu.VMEM((n, rows, ecols), BF),
            pltpu.VMEM((n_t, n, share, lcols), BF),
            pltpu.VMEM((n_t, share, width), BF),
            pltpu.VMEM((n_t, share, width), BF),
            pltpu.VMEM((n_t, share, lcols), BF),
            pltpu.VMEM((n_t, share, lcols), BF),
            pltpu.VMEM((rows, qcols), F32),
            pltpu.VMEM((rows, lcols), F32),
            pltpu.VMEM((share, width), BF),
            pltpu.VMEM((n, 8, wcol + ccol), F32),
            pltpu.VMEM((n, 8, wcol + ccol), F32),
            pltpu.VMEM((n_t, 8, wcol + ccol), F32),
            dma((6,)),
            dma((7, 2, n)),
            dma((7, n)),
            dma((n,)),
            dma((n,)),
            dma((6, n)),
            dma((6, n)),
            dma((4, n_t)),
            dma((4, n_t)),
            dma((n_t,)),
            dma((n_t,)),
            dma((n_t, n)),
            dma((n_t, n)),
        ],
        compiler_params=pltpu.CompilerParams(
            collective_id=0, has_side_effects=True, vmem_limit_bytes=60 * 1024 * 1024
        ),
    )(
        saved[0], top_grad, gain, compressed_gain, w_query[0], w_latent[0].T,
        expand_weight[0], w_output[0], cosine, sine,
    )
    parts = (ig, gg, gq, gl, glg, ge, go)
    ig, gg, gq, gl, glg, ge, go = pl.pallas_call(
        hand_over,
        name="hand_over",
        out_shape=tuple(shape(p.shape, p.dtype) for p in parts),
        in_specs=[vm] * 7,
        out_specs=(vm,) * 7,
    )(*parts)
    return ig[None], gg, gq[None], gl.T[None], glg, ge[None], go[None]


def choose(saved, top_grad, gain, w_query, w_latent, compressed_gain, expand_weight, w_output):
    arrays = (saved, top_grad, gain, w_query, w_latent, compressed_gain, expand_weight, w_output)
    n_t = lax.axis_size("tensor")
    fits = (
        lax.axis_size("dp") > 1
        and n_t % 2 == 0
        and w_query.shape[2] == 2 * (NOPE + ROPE)
        and gain.shape[1] % 128 == 0
        and compressed_gain.shape[1] % 128 == 0
        and saved.shape[2] % (16 * n_t) == 0
    )
    return section_step(*arrays) if fits else shards(*arrays)


def solution(mesh):
    in_specs = (
        P("pipe", None, "dp", None),
        P(None, "dp", None),
        P("pipe", "dp"),
        P("pipe", "dp", "tensor"),
        P("pipe", "dp", None),
        P("pipe", "dp"),
        P("pipe", "dp", "tensor"),
        P("pipe", "tensor", "dp"),
    )
    out_specs = (
        P("pipe", None, ("dp", "tensor"), None),
        P("pipe", "dp"),
        P("pipe", "dp", "tensor"),
        P("pipe", "dp", None),
        P("pipe", "dp"),
        P("pipe", "dp", "tensor"),
        P("pipe", "tensor", "dp"),
    )
    return jax.shard_map(choose, mesh=mesh, in_specs=in_specs, out_specs=out_specs, check_vma=False)
```
